128 devices in a mesh: band: 8 (over y, core), tile: 16 (over z, x).
Axes of the slice: x: 4, y: 4, z: 4, core: 2. Of those that a mesh axis runs over, the one named last changes fastest.
Arguments:
- patches: bfloat16 [1048576, 128], P(('band', 'tile')), may hold values from -6 to 6
- pair_patch: int32 [16384], P(('band', 'tile')), may hold values from 0 to 63
- pair_atm: int32 [16384], P(('band', 'tile')), may hold values from 0 to 16383, as said below
- numerators: int32 [16384, 128, 32], P(('band', 'tile')), may hold values from 0 to 16777215
- counts: int32 [128], P(('band', 'tile')), may hold values from 32 to 128, as said below
Outputs:
- atmosphere: float32 [524288, 128], P(('band', 'tile'))
The draws below stay inside these ranges and needn't reach their ends.
Inputs may be any that keep to these rules, and one draw needn't show every extreme that they name: Block pair_atm[g] is owned by device pair_atm[g] // 128 (band-major device order). Every live pair of device (b, t) targets an owner in band b (any tile) or one of (b - 1, t), (b + 1, t). Among one device's live pairs at most 32 target one owner and at most 16 distinct blocks of one owner; both are reached on some device in every draw. Slots that are not live hold arbitrary blocks in range. `counts`: the value 128 occurs on some device in every draw.
All inputs are finite; a program needn't handle non-finite values.
Results may differ from the reference program's by a relative error of at most 0.0026.
Values sent between devices are 32-bit elements; how exact they have to be, the bound alone decides.
A program may use at most 64 MiB of HBM per device.

```python
import jax
import jax.numpy as jnp
from jax import lax

FLUX = 128
PATCH_BLK = 128
CELL_BLK = 32
PBLK_DEV = 64
CELLS_DEV = 4096
PATCHES = 1048576
ALL_PAIRS = 16384
N_BAND = 8
N_TILE = 16


def shuffle_one(subkey):
    return jax.random.permutation(subkey, 2 * PBLK_DEV)


def routing(key):
    base_key = jax.random.fold_in(key, 7)
    subkeys = jax.random.split(base_key, 7)
    devices_all = N_BAND * N_TILE
    pairs_here = 2 * PBLK_DEV
    capacity = PBLK_DEV // 2
    distinct = capacity // 2
    blocks_owned = CELLS_DEV // CELL_BLK
    window = blocks_owned // distinct
    device_ids = jnp.arange(devices_all)
    band_of = (device_ids // N_TILE)[:, None]
    tile_of = (device_ids % N_TILE)[:, None]
    fullest_band = jax.random.randint(subkeys[4], (), 1, N_BAND - 1)
    fullest_tile = jax.random.randint(subkeys[5], (), 0, N_TILE)
    fullest = fullest_band * N_TILE + fullest_tile
    offset_far = jax.random.randint(subkeys[6], (devices_all, 1), 1, N_TILE)
    offset_far = jnp.where(device_ids[:, None] == fullest, N_TILE // 2, offset_far)
    offset_edge = jnp.where(offset_far == N_TILE - 1, 1, offset_far + 1)
    position = jnp.arange(pairs_here)[None, :]
    group = jnp.broadcast_to(position // capacity, (devices_all, pairs_here))
    candidate = jnp.broadcast_to(position % distinct, (devices_all, pairs_here))
    target_band = band_of + jnp.where(group == 1, -1, jnp.where(group == 2, 1, 0))
    target_tile = tile_of + jnp.where(group == 0, offset_far, 0)
    low_edge = (group == 1) & (band_of == 0)
    high_edge = (group == 2) & (band_of == N_BAND - 1)
    at_edge = low_edge | high_edge
    target_band = jnp.where(at_edge, band_of, target_band)
    target_tile = jnp.where(at_edge, tile_of + offset_edge, target_tile) % N_TILE
    owner = target_band * N_TILE + target_tile
    anchor = jax.random.randint(subkeys[0], (devices_all, 4), 0, blocks_owned)
    offsets = jax.random.randint(subkeys[1], (devices_all, 4 * distinct), 0, window)
    anchor_pick = jnp.take_along_axis(anchor, group, axis=1)
    offset_pick = jnp.take_along_axis(offsets, group * distinct + candidate, axis=1)
    local_block = (anchor_pick + candidate * window + offset_pick) % blocks_owned
    global_block = owner * blocks_owned + local_block
    shuffles = jax.vmap(shuffle_one)(jax.random.split(subkeys[2], devices_all))
    global_block = jnp.take_along_axis(global_block, shuffles, axis=1)
    live_counts = jax.random.randint(subkeys[3], (devices_all,), pairs_here // 4, pairs_here + 1)
    live_counts = jnp.where(device_ids == fullest, pairs_here, live_counts)
    return (global_block.reshape(-1).astype(jnp.int32), live_counts.astype(jnp.int32))


def draw_pair_atm(key, part):
    return routing(key)[0]


def draw_counts(key, part):
    return routing(key)[1]


def touch_ends(values, stream_key, least, high):
    extent = values.shape
    index_at = [jax.random.randint(jax.random.fold_in(stream_key, axis), (), 0, extent[axis]) for axis in range(len(extent))]
    values = values.at[tuple(index_at)].set(least)
    longest = extent.index(max(extent))
    index_at[longest] = (index_at[longest] + 1) % extent[longest]
    return values.at[tuple(index_at)].set(high)


def steps_of(stream_key, dims, cuts, smallest, top_value):
    level, own = 1.0, jax.random.fold_in(stream_key, 6)
    for dim, blocks in cuts:
        steps = jnp.exp(jax.random.uniform(jax.random.fold_in(own, dim), (blocks,), jnp.float32, smallest / len(cuts), top_value / len(cuts)))
        level = level * jnp.repeat(steps, dims[dim] // blocks).reshape([-1 if axis == dim else 1 for axis in range(len(dims))])
    return level


def noise(own_key, shape, width, most, shards=(), held_as=jnp.bfloat16):
    loudness = steps_of(own_key, shape, shards, -0.22, 0.18) if shards else 1.0
    result = jax.random.normal(own_key, shape, jnp.float32) * width * loudness
    return jnp.minimum(jnp.maximum(result, -most), most).astype(held_as)


def setup_inputs(seed: int = 0) -> dict:
    key_list = jax.random.split(jax.random.key(seed), 6)
    return {
        "patches": noise(key_list[0], (PATCHES, FLUX), 1.0, 6.0, ((0, 128),)),
        "pair_patch": touch_ends(jax.random.randint(key_list[1], (ALL_PAIRS,), 0, PBLK_DEV), jax.random.fold_in(key_list[1], 1), 0, PBLK_DEV - 1).astype(jnp.int32),
        "pair_atm": draw_pair_atm(jax.random.fold_in(key_list[5], 71), 0),
        "numerators": touch_ends(jax.random.randint(key_list[3], (ALL_PAIRS, PATCH_BLK, CELL_BLK), 0, 16777216), jax.random.fold_in(key_list[3], 1), 0, 16777215).astype(jnp.int32),
        "counts": draw_counts(jax.random.fold_in(key_list[5], 71), 0),
    }


SCALE = 2.0 ** -27


def reference(patches, pair_patch, pair_atm, numerators, counts):
    devices_all = N_BAND * N_TILE
    pairs_here = 2 * PBLK_DEV
    blocks_owned = CELLS_DEV // CELL_BLK
    grouped = patches.reshape(devices_all, PBLK_DEV, PATCH_BLK, FLUX)
    patch_table = pair_patch.reshape(devices_all, pairs_here)
    atm_table = pair_atm.reshape(devices_all, pairs_here)
    numer_table = numerators.reshape(devices_all, pairs_here, PATCH_BLK, CELL_BLK)

    def add_device(accumulated, inputs):
        dev_blocks, patch_index, atm_index, numerator, live_count = inputs
        live_mask = (jnp.arange(pairs_here) < live_count).astype(jnp.float32)
        weight = (numerator.astype(jnp.float32) * SCALE).astype(jnp.bfloat16)
        weight = lax.optimization_barrier(weight).astype(jnp.float32)
        chosen = dev_blocks[patch_index.astype(jnp.int32)].astype(jnp.float32)
        partial_value = jnp.einsum("jpa,jpf->jaf", weight, chosen, precision=lax.Precision.HIGHEST)
        partial_value = partial_value * live_mask[:, None, None]
        return accumulated.at[atm_index.astype(jnp.int32)].add(partial_value), None

    initial = jnp.zeros((devices_all * blocks_owned, CELL_BLK, FLUX), jnp.float32)
    accumulated, unused = lax.scan(add_device, initial, (grouped, patch_table, atm_table, numer_table, counts))
    return accumulated.reshape(devices_all * blocks_owned * CELL_BLK, FLUX)
```

```python
import functools

import jax
import jax.numpy as jnp
from jax import lax
from jax.experimental import pallas as pl
from jax.experimental.pallas import tpu as pltpu
from jax.sharding import PartitionSpec as P

CELLS_DEV = 4096
SCALE = 2.0 ** (-27)

TILES = 16
BANDS = 8
PAIRS = 128
CELLS = 32
LANES = 128
BLOCKS = 128
NEAR = 16
FAR0 = 3 * NEAR
NC = 32
DC = 72
PIECE = CELLS // TILES
MESH = pl.DeviceIdType.MESH
F32, BF16, I32 = jnp.float32, jnp.bfloat16, jnp.int32


def iota(shape, axis):
    return lax.broadcasted_iota(I32, shape, axis)


def split(value):
    high = value.astype(BF16)
    return high, (value - high.astype(F32)).astype(BF16)


def exchange_kernel(
    counts_ref, patch_ref, atm_ref, num_hbm, patches_hbm,
    far_ref, near_ref, place_ref, flag_ref,
    num_v, pat_v, part, send_far, send_up, send_down, relay, stacked, parcel,
    note, notes, alarm, alarms,
    in_sem, note_send, note_recv, r_send, r_recv, q_send, q_recv,
    near_send, near_recv, alarm_send, alarm_recv,
):
    band, tile = lax.axis_index("band"), lax.axis_index("tile")
    chunks = in_sem.shape[0] - 1
    rows = PAIRS // chunks

    def tile_at(k):
        return lax.rem(tile + k, TILES)

    def band_at(k):
        return lax.rem(band + k, BANDS)

    pat_copy = pltpu.make_async_copy(patches_hbm, pat_v, in_sem.at[chunks])
    pat_copy.start()
    num_copies = [
        pltpu.make_async_copy(
            num_hbm.at[pl.ds(i * rows, rows)], num_v.at[pl.ds(i * rows, rows)], in_sem.at[i]
        )
        for i in range(chunks)
    ]
    for copy in num_copies:
        copy.start()

    barrier = pltpu.get_barrier_semaphore()

    @pl.loop(1, TILES)
    def _(k):
        pl.semaphore_signal(barrier, inc=1, device_id={"tile": tile_at(k)}, device_id_type=MESH)

    @pl.loop(1, BANDS)
    def _(k):
        pl.semaphore_signal(barrier, inc=1, device_id={"band": band_at(k)}, device_id_type=MESH)

    lane, sub = iota((PAIRS, LANES), 1), iota((PAIRS, LANES), 0)
    lane1 = iota((1, LANES), 1)

    def column(row):
        return jnp.sum(jnp.where(lane == sub, row, 0.0), axis=1, keepdims=True)

    atm = atm_ref[...]
    live = lane1 < counts_ref[0]
    owner = atm >> 7
    me = band * TILES + tile
    base = jnp.where(
        owner == me,
        0,
        jnp.where(owner == me + TILES, NEAR, jnp.where(owner == me - TILES, 2 * NEAR, FAR0)),
    ).astype(F32)
    key = jnp.where(live, atm, -1).astype(F32)
    key_c, base_c = column(key), column(base)
    same = (key_c == key) & (key >= 0.0)
    earlier = jnp.sum(jnp.where(same & (sub < lane), 1.0, 0.0), axis=0, keepdims=True)
    first = jnp.where(live & (earlier == 0.0), 1.0, 0.0)
    first_c = column(first)
    ahead = (first_c > 0.0) & (base_c == base) & (key_c < key)
    rank = jnp.sum(jnp.where(ahead, 1.0, 0.0), axis=0, keepdims=True)
    slot = jnp.where(live, base + rank, -1.0)
    slot_c = column(slot).astype(I32)
    leads = first_c > 0.0
    key_i = key_c.astype(I32)
    far_lane = slot_c - FAR0 + NC * lax.rem(tile, 4)
    in_far = leads & (slot_c >= FAR0) & (slot_c < FAR0 + NC)
    far_label = (key_i - band * (TILES * BLOCKS) + 1).astype(F32)
    far_row = jnp.sum(jnp.where(in_far & (far_lane == lane), far_label, 0.0), axis=0, keepdims=True)
    in_near = leads & (slot_c < FAR0) & (slot_c == lane)
    near_label = ((key_i & (BLOCKS - 1)) + 1).astype(F32)
    near_row = jnp.sum(jnp.where(in_near, near_label, 0.0), axis=0, keepdims=True)
    n_far = jnp.sum(jnp.where(base == FAR0, first, 0.0), axis=1, keepdims=True)
    note[0:1, :] = far_row
    note[1:2, :] = jnp.where(lane1 == LANES - 1, n_far, near_row)

    @pl.when(band == 0)
    def _():
        notes[TILES] = jnp.zeros((2, LANES), F32)
        near_ref[1] = jnp.zeros((CELLS, NEAR, LANES), F32)

    @pl.when(band == BANDS - 1)
    def _():
        notes[TILES + 1] = jnp.zeros((2, LANES), F32)
        near_ref[2] = jnp.zeros((CELLS, NEAR, LANES), F32)

    pl.semaphore_wait(barrier, TILES + BANDS - 2)

    def note_to(k):
        return pltpu.make_async_remote_copy(
            src_ref=note, dst_ref=notes.at[tile], send_sem=note_send.at[tile_at(k)],
            recv_sem=note_recv.at[tile], device_id={"tile": tile_at(k)}, device_id_type=MESH,
        )

    def note_from(k):
        source = tile_at(TILES - k)
        return pltpu.make_async_remote_copy(
            src_ref=note, dst_ref=notes.at[source], send_sem=note_send.at[source],
            recv_sem=note_recv.at[source], device_id={"tile": source}, device_id_type=MESH,
        )

    def note_up():
        return pltpu.make_async_remote_copy(
            src_ref=note, dst_ref=notes.at[TILES], send_sem=note_send.at[TILES],
            recv_sem=note_recv.at[TILES], device_id={"band": band_at(1)}, device_id_type=MESH,
        )

    def note_down():
        return pltpu.make_async_remote_copy(
            src_ref=note, dst_ref=notes.at[TILES + 1], send_sem=note_send.at[TILES + 1],
            recv_sem=note_recv.at[TILES + 1], device_id={"band": band_at(BANDS - 1)},
            device_id_type=MESH,
        )

    @pl.loop(1, TILES)
    def _(k):
        note_to(k).start()

    @pl.when(band < BANDS - 1)
    def _():
        note_up().start()

    @pl.when(band > 0)
    def _():
        note_down().start()

    notes[tile] = note[...]

    pat_copy.wait()
    for i in range(chunks):
        num_copies[i].wait()

        @pl.loop(0, rows, unroll=8)
        def _(j):
            g = i * rows + j
            weight = num_v[g].astype(F32).astype(BF16)
            part[pl.ds(g, CELLS, stride=PAIRS), :] = jnp.dot(
                weight, pat_v[patch_ref[g]], preferred_element_type=F32
            )

    slot_sub = iota((FAR0 + NC, LANES), 0)
    pick = jnp.where(slot.astype(I32) == slot_sub, SCALE, 0.0).astype(BF16)
    pick2 = jnp.concatenate([pick, pick], axis=1)

    def slots_of(m):
        both = part[pl.ds(m * PIECE * PAIRS, PIECE * PAIRS), :]
        wide = jnp.concatenate([both[:PAIRS], both[PAIRS:]], axis=1)
        total = jnp.dot(
            pick2, jnp.concatenate(split(wide), axis=0), preferred_element_type=F32
        )
        for c in range(PIECE):
            here = total[:, c * LANES : (c + 1) * LANES]
            near_ref[0, m * PIECE + c] = here[:NEAR]
            send_up[m * PIECE + c] = here[NEAR : 2 * NEAR]
            send_down[m * PIECE + c] = here[2 * NEAR : FAR0]
            send_far[m, c] = here[FAR0:]

    def far_to(k):
        return pltpu.make_async_remote_copy(
            src_ref=send_far.at[tile_at(k)], dst_ref=relay.at[tile], send_sem=r_send.at[tile_at(k)],
            recv_sem=r_recv.at[tile], device_id={"tile": tile_at(k)}, device_id_type=MESH,
        )

    def far_from(k):
        source = tile_at(TILES - k)
        return pltpu.make_async_remote_copy(
            src_ref=send_far.at[source], dst_ref=relay.at[source], send_sem=r_send.at[source],
            recv_sem=r_recv.at[source], device_id={"tile": source}, device_id_type=MESH,
        )

    @pl.loop(1, TILES)
    def _(k):
        slots_of(tile_at(k))
        far_to(k).start()

    slots_of(tile)
    relay[tile] = send_far[tile]

    def near_up():
        return pltpu.make_async_remote_copy(
            src_ref=send_up, dst_ref=near_ref.at[1], send_sem=near_send.at[0],
            recv_sem=near_recv.at[0], device_id={"band": band_at(1)}, device_id_type=MESH,
        )

    def near_down():
        return pltpu.make_async_remote_copy(
            src_ref=send_down, dst_ref=near_ref.at[2], send_sem=near_send.at[1],
            recv_sem=near_recv.at[1], device_id={"band": band_at(BANDS - 1)}, device_id_type=MESH,
        )

    @pl.when(band < BANDS - 1)
    def _():
        near_up().start()

    @pl.when(band > 0)
    def _():
        near_down().start()

    @pl.loop(1, TILES)
    def _(k):
        note_from(k).wait_recv()

    quarters = []
    for q in range(4):
        quarters.append(
            notes[4 * q, 0:1, :] + notes[4 * q + 1, 0:1, :]
            + notes[4 * q + 2, 0:1, :] + notes[4 * q + 3, 0:1, :]
        )
    label = jnp.concatenate(quarters, axis=1).astype(I32)
    entries = TILES * NC
    filled = label > 0
    label = label - 1
    goes_to, block = label >> 7, label & (BLOCKS - 1)
    is_block = filled & (iota((BLOCKS, entries), 0) == block)
    block_hot = jnp.where(is_block, 1.0, 0.0).astype(BF16)
    owner_hot = jnp.where(
        filled & (iota((TILES, entries), 0) == goes_to), 1.0, 0.0
    ).astype(BF16)
    hits = lax.dot_general(
        block_hot, owner_hot, (((1,), (1,)), ((), ())), preferred_element_type=F32
    )
    taken = jnp.where(hits > 0.0, 1.0, 0.0)
    below = jnp.where(lane < sub, 1.0, 0.0).astype(BF16)
    order = jnp.dot(below, taken.astype(BF16), preferred_element_type=F32)
    spread = jnp.dot(order.astype(BF16), owner_hot, preferred_element_type=F32)
    depth = jnp.sum(jnp.where(is_block, spread, 0.0), axis=0, keepdims=True).astype(I32)
    goal = jnp.where(filled & (depth < DC), goes_to * DC + depth, -1)

    most_far = notes[0, 1:2, :]
    for s in range(1, TILES):
        most_far = jnp.maximum(most_far, notes[s, 1:2, :])
    over_far = jnp.max(
        jnp.where(lane1 == LANES - 1, most_far - NC, 0.0), axis=1, keepdims=True
    )
    load = jnp.sum(taken, axis=0, keepdims=True)
    over_load = jnp.max(load - DC, axis=1, keepdims=True)
    alarm[...] = jnp.broadcast_to(
        jnp.where((over_far > 0.0) | (over_load > 0.0), 1.0, 0.0), (1, LANES)
    )

    def alarm_to(k):
        return pltpu.make_async_remote_copy(
            src_ref=alarm, dst_ref=alarms.at[band], send_sem=alarm_send.at[band_at(k)],
            recv_sem=alarm_recv.at[band], device_id={"band": band_at(k)}, device_id_type=MESH,
        )

    def alarm_from(k):
        source = band_at(BANDS - k)
        return pltpu.make_async_remote_copy(
            src_ref=alarm, dst_ref=alarms.at[source], send_sem=alarm_send.at[source],
            recv_sem=alarm_recv.at[source], device_id={"band": source}, device_id_type=MESH,
        )

    @pl.loop(1, BANDS)
    def _(k):
        alarm_to(k).start()

    alarms[band] = alarm[...]

    @pl.when(band > 0)
    def _():
        note_up().wait_recv()

    @pl.when(band < BANDS - 1)
    def _():
        note_down().wait_recv()

    near_labels = jnp.where(
        lane1 < NEAR,
        note[1:2, :],
        jnp.where(lane1 < 2 * NEAR, notes[TILES, 1:2, :], notes[TILES + 1, 1:2, :]),
    )
    mine = iota((BLOCKS, TILES), 1) == tile
    my_taken = jnp.sum(jnp.where(mine, taken, 0.0), axis=1, keepdims=True)
    my_order = jnp.sum(jnp.where(mine, order, 0.0), axis=1, keepdims=True).astype(I32)
    is_near = (lane < FAR0) & (near_labels.astype(I32) == sub + 1)
    is_far = (lane >= FAR0) & (lane < FAR0 + DC) & (my_taken > 0.0) & (my_order == lane - FAR0)
    place_ref[...] = jnp.where(is_near | is_far, 1.0, 0.0)

    @pl.loop(1, TILES)
    def _(k):
        far_from(k).wait_recv()

    for c in range(PIECE):
        high, low = split(relay[:, c].reshape(entries, LANES))
        stacked[:entries, c * LANES : (c + 1) * LANES] = high
        stacked[entries:, c * LANES : (c + 1) * LANES] = low
    depth_sub = iota((DC, entries), 0)

    def blocks_of(owner_tile):
        hot = jnp.where(depth_sub + owner_tile * DC == goal, 1.0, 0.0).astype(BF16)
        return jnp.dot(
            jnp.concatenate([hot, hot], axis=1), stacked[...], preferred_element_type=F32
        )

    def parcel_to(k):
        return pltpu.make_async_remote_copy(
            src_ref=parcel.at[tile_at(k)], dst_ref=far_ref.at[tile], send_sem=q_send.at[tile_at(k)],
            recv_sem=q_recv.at[tile], device_id={"tile": tile_at(k)}, device_id_type=MESH,
        )

    def parcel_from(k):
        source = tile_at(TILES - k)
        return pltpu.make_async_remote_copy(
            src_ref=parcel.at[source], dst_ref=far_ref.at[source], send_sem=q_send.at[source],
            recv_sem=q_recv.at[source], device_id={"tile": source}, device_id_type=MESH,
        )

    @pl.loop(1, TILES)
    def _(k):
        total = blocks_of(tile_at(k))
        for c in range(PIECE):
            parcel[tile_at(k), c] = total[:, c * LANES : (c + 1) * LANES]
        parcel_to(k).start()

    own = blocks_of(tile)
    for c in range(PIECE):
        far_ref[tile, c] = own[:, c * LANES : (c + 1) * LANES]

    @pl.loop(1, BANDS)
    def _(k):
        alarm_from(k).wait_recv()

    flag_ref[0] = jnp.max(alarms[...]).astype(I32)

    @pl.when(band > 0)
    def _():
        near_up().wait_recv()
        note_down().wait_send()
        near_down().wait_send()

    @pl.when(band < BANDS - 1)
    def _():
        near_down().wait_recv()
        note_up().wait_send()
        near_up().wait_send()

    @pl.loop(1, BANDS)
    def _(k):
        alarm_to(k).wait_send()

    @pl.loop(1, TILES)
    def _(k):
        note_to(k).wait_send()
        far_to(k).wait_send()
        parcel_from(k).wait_recv()

    @pl.loop(1, TILES)
    def _(k):
        parcel_to(k).wait_send()


def exchange(patches, pair_patch, pair_atm, numerators, counts):
    vmem = pl.BlockSpec(memory_space=pltpu.VMEM)
    smem = pl.BlockSpec(memory_space=pltpu.SMEM)
    anywhere = pl.BlockSpec(memory_space=pl.ANY)
    dma = pltpu.SemaphoreType.DMA
    return pl.pallas_call(
        exchange_kernel,
        out_shape=(
            jax.ShapeDtypeStruct((TILES, PIECE, DC, LANES), F32),
            jax.ShapeDtypeStruct((3, CELLS, NEAR, LANES), F32),
            jax.ShapeDtypeStruct((BLOCKS, LANES), F32),
            jax.ShapeDtypeStruct((1,), I32),
        ),
        in_specs=[smem, smem, vmem, anywhere, anywhere],
        out_specs=(vmem, vmem, vmem, smem),
        scratch_shapes=[
            pltpu.VMEM((PAIRS, CELLS, LANES), I32),
            pltpu.VMEM((PAIRS // 2, LANES, LANES), BF16),
            pltpu.VMEM((CELLS * PAIRS, LANES), F32),
            pltpu.VMEM((TILES, PIECE, NC, LANES), F32),
            pltpu.VMEM((CELLS, NEAR, LANES), F32),
            pltpu.VMEM((CELLS, NEAR, LANES), F32),
            pltpu.VMEM((TILES, PIECE, NC, LANES), F32),
            pltpu.VMEM((2 * TILES * NC, PIECE * LANES), BF16),
            pltpu.VMEM((TILES, PIECE, DC, LANES), F32),
            pltpu.VMEM((2, LANES), F32),
            pltpu.VMEM((TILES + 2, 2, LANES), F32),
            pltpu.VMEM((1, LANES), F32),
            pltpu.VMEM((BANDS, 1, LANES), F32),
            dma((5,)),
            dma((TILES + 2,)), dma((TILES + 2,)),
            dma((TILES,)), dma((TILES,)),
            dma((TILES,)), dma((TILES,)),
            dma((2,)), dma((2,)),
            dma((BANDS,)), dma((BANDS,)),
        ],
        compiler_params=pltpu.CompilerParams(
            collective_id=0, has_side_effects=True, vmem_limit_bytes=40 * 2**20
        ),
        name="exchange",
    )(
        counts,
        pair_patch,
        pair_atm.reshape(1, PAIRS),
        numerators.transpose(0, 2, 1),
        patches.reshape(-1, LANES, LANES),
    )


def place_kernel(far_ref, near_ref, place_ref, out_ref):
    put = place_ref[...].astype(BF16)
    put2 = jnp.concatenate([put, put], axis=1)
    rest = jnp.zeros((LANES - FAR0 - DC, PIECE * LANES), F32)

    @pl.loop(0, TILES)
    def _(m):
        groups = [
            jnp.concatenate([near_ref[i, m * PIECE + c] for c in range(PIECE)], axis=1)
            for i in range(3)
        ]
        groups.append(jnp.concatenate([far_ref[m, c] for c in range(PIECE)], axis=1))
        groups.append(rest)
        high, low = split(jnp.concatenate(groups, axis=0))
        total = jnp.dot(
            put2, jnp.concatenate([high, low], axis=0), preferred_element_type=F32
        )
        for c in range(PIECE):
            out_ref[pl.ds(m * PIECE + c, BLOCKS, stride=CELLS), :] = total[
                :, c * LANES : (c + 1) * LANES
            ]


def place(far, near, put):
    vmem = pl.BlockSpec(memory_space=pltpu.VMEM)
    return pl.pallas_call(
        place_kernel,
        out_shape=jax.ShapeDtypeStruct((BLOCKS * CELLS, LANES), F32),
        in_specs=[vmem, vmem, vmem],
        out_specs=vmem,
        compiler_params=pltpu.CompilerParams(vmem_limit_bytes=40 * 2**20),
        name="place",
    )(far, near, put)


def shifted(value, axis, steps):
    count = lax.axis_size(axis)
    first, last = (max(0, -steps), min(count, count - steps))
    return lax.ppermute(value, axis, [(source, source + steps) for source in range(first, last)])


def slot_ranks(owners, blocks_local, live_pairs):
    position = jnp.arange(owners.shape[0])
    earlier = position[None, :] < position[:, None]
    both_live = live_pairs[None, :] & live_pairs[:, None]
    same_owner = (owners[:, None] == owners[None, :]) & both_live
    same_block = same_owner & (blocks_local[:, None] == blocks_local[None, :])
    leading = jnp.logical_not(jnp.any(same_block & earlier, axis=1))
    leader_rank = jnp.sum((same_owner & earlier & leading[None, :]).astype(jnp.int32), axis=1)
    first_match = same_block & leading[None, :]
    return jnp.sum(jnp.where(first_match, leader_rank[None, :], 0), axis=1)


def pack(flattened, rows_index, selected, blocks_local, rows_total):
    onehot = (rows_index[None, :] == jnp.arange(rows_total)[:, None]) & selected[None, :]
    payload = jnp.dot(onehot.astype(jnp.float32), flattened, precision=lax.Precision.HIGHEST)
    labels = jnp.max(jnp.where(onehot, blocks_local[None, :], -1), axis=1)
    return (payload, labels)


def unpack(payload, labels, blocks_owned):
    onehot = (labels[None, :] == jnp.arange(blocks_owned)[:, None]).astype(jnp.float32)
    return jnp.dot(onehot, payload, precision=lax.Precision.HIGHEST)


def along_band(parcel, offset_by):
    return shifted((parcel[0], parcel[1]), "band", offset_by)


def long_route(patches, pair_patch, pair_atm, numerators, counts):
    pairs_here, patch_rows, cell_rows = numerators.shape
    flux_width = patches.shape[1]
    blocks_owned = CELLS_DEV // cell_rows
    capacity = pairs_here // 4
    grouped = patches.reshape(-1, patch_rows, flux_width)
    live_pairs = jnp.arange(pairs_here) < counts[0]
    weight = (numerators.astype(jnp.float32) * SCALE).astype(jnp.bfloat16)
    chosen = grouped[pair_patch]
    partial_value = jnp.einsum("jpa,jpf->jaf", weight, chosen, preferred_element_type=jnp.float32)
    flattened = partial_value.reshape(pairs_here, cell_rows * flux_width)
    owners = pair_atm // blocks_owned
    blocks_local = pair_atm % blocks_owned
    slot_rank = slot_ranks(owners, blocks_local, live_pairs)
    bucket_size = capacity // 2
    tile_count = lax.axis_size("tile")
    band_now = lax.axis_index("band")
    tile_now = lax.axis_index("tile")
    owner_band = owners // tile_count
    owner_tile = owners % tile_count
    in_band = live_pairs & (owner_band == band_now)
    rows_index = jnp.where(in_band, owner_tile * bucket_size + slot_rank, -1)
    payload, labels = pack(flattened, rows_index, in_band, blocks_local, tile_count * bucket_size)

    def bucket(target):
        addressed = live_pairs & (owners == target)
        target_rows = jnp.where(addressed, slot_rank, -1)
        return pack(flattened, target_rows, addressed, blocks_local, bucket_size)

    upper_index = (band_now + 1) * tile_count + tile_now
    lower_index = (band_now - 1) * tile_count + tile_now
    from_below = along_band(bucket(upper_index), 1)
    from_above = along_band(bucket(lower_index), -1)
    band_payload = jnp.concatenate([from_below[0], from_above[0]], axis=0)
    band_labels = jnp.concatenate([from_below[1], from_above[1]], axis=0)
    payload, labels = (
        lax.all_to_all(
            payload.reshape(tile_count, bucket_size, -1),
            "tile",
            split_axis=0,
            concat_axis=0,
            tiled=True,
        ),
        lax.all_to_all(
            labels.reshape(tile_count, bucket_size), "tile", split_axis=0, concat_axis=0, tiled=True
        ),
    )
    payload = jnp.concatenate([payload.reshape(tile_count * bucket_size, -1), band_payload], axis=0)
    labels = jnp.concatenate([labels.reshape(-1), band_labels], axis=0)
    summed = unpack(payload, labels, blocks_owned)
    return summed.reshape(blocks_owned * cell_rows, flux_width)


def per_device(patches, pair_patch, pair_atm, numerators, counts):
    far, near, put, flag = exchange(patches, pair_patch, pair_atm, numerators, counts)
    return lax.cond(
        flag[0] == 0,
        lambda: place(far, near, put),
        lambda: long_route(patches, pair_patch, pair_atm, numerators, counts),
    )


def solution(mesh):
    placed = (
        P(("band", "tile"), None),
        P(("band", "tile")),
        P(("band", "tile")),
        P(("band", "tile"), None, None),
        P(("band", "tile")),
    )
    return jax.shard_map(
        per_device, mesh=mesh, in_specs=placed, out_specs=P(("band", "tile"), None), check_vma=False
    )
```

```python
import functools

import jax
import jax.numpy as jnp
from jax import lax
from jax.experimental import pallas as pl
from jax.experimental.pallas import tpu as pltpu
from jax.sharding import PartitionSpec as P

CELLS_DEV = 4096
SCALE = 2.0 ** (-27)

TILES = 16
BANDS = 8
PAIRS = 128
CELLS = 32
LANES = 128
BLOCKS = 128
NEAR = 16
FAR0 = 3 * NEAR
NC = 32
DC = 80
NC_MID, DC_MID = 16, 72
PIECE = CELLS // TILES
MESH = pl.DeviceIdType.MESH
F32, BF16, I32 = jnp.float32, jnp.bfloat16, jnp.int32


def iota(shape, axis):
    return lax.broadcasted_iota(I32, shape, axis)


def split(value):
    high = value.astype(BF16)
    return high, (value - high.astype(F32)).astype(BF16)


def exchange_kernel(
    counts_ref, patch_hbm, atm_hbm, num_hbm, patches_hbm,
    out_ref, flag_ref,
    patch_ref, atm_ref, num_v, pat_v, part, send_far, send_up, send_down, relay, stacked,
    parcel, far_ref, near_ref, note, notes, alarm, alarms,
    in_sem, note_send, note_recv, r_send, r_recv, q_send, q_recv,
    near_send, near_recv, alarm_send, alarm_recv,
):
    band, tile = lax.axis_index("band"), lax.axis_index("tile")
    edge = (band == 0) | (band == BANDS - 1)
    chunks = in_sem.shape[0] - 3
    rows = PAIRS // chunks

    def tile_at(k):
        return lax.rem(tile + k, TILES)

    def band_at(k):
        return lax.rem(band + k, BANDS)

    def each_size(body):
        @pl.when(edge)
        def _():
            body(NC, DC)

        @pl.when(jnp.logical_not(edge))
        def _():
            body(NC_MID, DC_MID)

    atm_copy = pltpu.make_async_copy(atm_hbm, atm_ref, in_sem.at[chunks + 1])
    atm_copy.start()
    patch_copy = pltpu.make_async_copy(patch_hbm, patch_ref, in_sem.at[chunks + 2])
    patch_copy.start()
    pat_copy = pltpu.make_async_copy(patches_hbm, pat_v, in_sem.at[chunks])
    pat_copy.start()
    num_copies = [
        pltpu.make_async_copy(
            num_hbm.at[pl.ds(i * rows, rows)], num_v.at[pl.ds(i * rows, rows)], in_sem.at[i]
        )
        for i in range(chunks)
    ]
    for copy in num_copies:
        copy.start()

    barrier = pltpu.get_barrier_semaphore()

    @pl.loop(1, TILES)
    def _(k):
        pl.semaphore_signal(barrier, inc=1, device_id={"tile": tile_at(k)}, device_id_type=MESH)

    @pl.loop(1, BANDS)
    def _(k):
        pl.semaphore_signal(barrier, inc=1, device_id={"band": band_at(k)}, device_id_type=MESH)

    lane, sub = iota((PAIRS, LANES), 1), iota((PAIRS, LANES), 0)
    lane1 = iota((1, LANES), 1)

    def column(row):
        return jnp.sum(jnp.where(lane == sub, row, 0.0), axis=1, keepdims=True)

    atm_copy.wait()
    atm = atm_ref[...]
    live = lane1 < counts_ref[0]
    owner = atm >> 7
    me = band * TILES + tile
    base = jnp.where(
        owner == me,
        0,
        jnp.where(owner == me + TILES, NEAR, jnp.where(owner == me - TILES, 2 * NEAR, FAR0)),
    ).astype(F32)
    key = jnp.where(live, atm, -1).astype(F32)
    key_c, base_c = column(key), column(base)
    same = (key_c == key) & (key >= 0.0)
    earlier = jnp.sum(jnp.where(same & (sub < lane), 1.0, 0.0), axis=0, keepdims=True)
    first = jnp.where(live & (earlier == 0.0), 1.0, 0.0)
    first_c = column(first)
    ahead = (first_c > 0.0) & (base_c == base) & (key_c < key)
    rank = jnp.sum(jnp.where(ahead, 1.0, 0.0), axis=0, keepdims=True)
    slot = jnp.where(live, base + rank, -1.0)
    slot_c = column(slot).astype(I32)
    leads = first_c > 0.0
    key_i = key_c.astype(I32)
    far_lane = slot_c - FAR0 + NC * lax.rem(tile, 4)
    in_far = leads & (slot_c >= FAR0) & (slot_c < FAR0 + NC)
    far_label = (key_i - band * (TILES * BLOCKS) + 1).astype(F32)
    far_row = jnp.sum(jnp.where(in_far & (far_lane == lane), far_label, 0.0), axis=0, keepdims=True)
    in_near = leads & (slot_c < FAR0) & (slot_c == lane)
    near_label = ((key_i & (BLOCKS - 1)) + 1).astype(F32)
    near_row = jnp.sum(jnp.where(in_near, near_label, 0.0), axis=0, keepdims=True)
    n_far = jnp.sum(jnp.where(base == FAR0, first, 0.0), axis=1, keepdims=True)
    note[0:1, :] = far_row
    note[1:2, :] = jnp.where(lane1 == LANES - 1, n_far, near_row)

    @pl.when(band == 0)
    def _():
        notes[TILES] = jnp.zeros((2, LANES), F32)
        near_ref[1] = jnp.zeros((CELLS, NEAR, LANES), F32)

    @pl.when(band == BANDS - 1)
    def _():
        notes[TILES + 1] = jnp.zeros((2, LANES), F32)
        near_ref[2] = jnp.zeros((CELLS, NEAR, LANES), F32)

    @pl.when(jnp.logical_not(edge))
    def _():
        relay[:, :, NC_MID:] = jnp.zeros((TILES, PIECE, NC - NC_MID, LANES), F32)
        far_ref[:, :, DC_MID:] = jnp.zeros((TILES, PIECE, DC - DC_MID, LANES), F32)

    patch_copy.wait()
    pat_copy.wait()
    for i in range(chunks):
        num_copies[i].wait()

        @pl.loop(0, rows, unroll=8)
        def _(j):
            g = i * rows + j
            weight = num_v[g].astype(F32).astype(BF16)
            part[pl.ds(g, CELLS, stride=PAIRS), :] = jnp.dot(
                weight, pat_v[patch_ref[g]], preferred_element_type=F32
            )

    pl.semaphore_wait(barrier, TILES + BANDS - 2)

    def note_to(k):
        return pltpu.make_async_remote_copy(
            src_ref=note, dst_ref=notes.at[tile], send_sem=note_send.at[tile_at(k)],
            recv_sem=note_recv.at[tile], device_id={"tile": tile_at(k)}, device_id_type=MESH,
        )

    def note_from(k):
        source = tile_at(TILES - k)
        return pltpu.make_async_remote_copy(
            src_ref=note, dst_ref=notes.at[source], send_sem=note_send.at[source],
            recv_sem=note_recv.at[source], device_id={"tile": source}, device_id_type=MESH,
        )

    def note_up():
        return pltpu.make_async_remote_copy(
            src_ref=note, dst_ref=notes.at[TILES], send_sem=note_send.at[TILES],
            recv_sem=note_recv.at[TILES], device_id={"band": band_at(1)}, device_id_type=MESH,
        )

    def note_down():
        return pltpu.make_async_remote_copy(
            src_ref=note, dst_ref=notes.at[TILES + 1], send_sem=note_send.at[TILES + 1],
            recv_sem=note_recv.at[TILES + 1], device_id={"band": band_at(BANDS - 1)},
            device_id_type=MESH,
        )

    @pl.loop(1, TILES)
    def _(k):
        note_to(k).start()

    @pl.when(band < BANDS - 1)
    def _():
        note_up().start()

    @pl.when(band > 0)
    def _():
        note_down().start()

    notes[tile] = note[...]

    slot_sub = iota((FAR0 + NC, LANES), 0)
    pick = jnp.where(slot.astype(I32) == slot_sub, SCALE, 0.0).astype(BF16)
    pick2 = jnp.concatenate([pick, pick], axis=1)

    def slots_of(m):
        both = part[pl.ds(m * PIECE * PAIRS, PIECE * PAIRS), :]
        wide = jnp.concatenate([both[:PAIRS], both[PAIRS:]], axis=1)
        total = jnp.dot(
            pick2, jnp.concatenate(split(wide), axis=0), preferred_element_type=F32
        )
        for c in range(PIECE):
            here = total[:, c * LANES : (c + 1) * LANES]
            near_ref[0, m * PIECE + c] = here[:NEAR]
            send_up[m * PIECE + c] = here[NEAR : 2 * NEAR]
            send_down[m * PIECE + c] = here[2 * NEAR : FAR0]
            send_far[m, c] = here[FAR0:]

    def far_to(k, c, n):
        return pltpu.make_async_remote_copy(
            src_ref=send_far.at[tile_at(k), c, pl.ds(0, n)], dst_ref=relay.at[tile, c, pl.ds(0, n)],
            send_sem=r_send.at[c, tile_at(k)], recv_sem=r_recv.at[c, tile],
            device_id={"tile": tile_at(k)}, device_id_type=MESH,
        )

    def far_from(k, c, n):
        source = tile_at(TILES - k)
        return pltpu.make_async_remote_copy(
            src_ref=send_far.at[source, c, pl.ds(0, n)], dst_ref=relay.at[source, c, pl.ds(0, n)],
            send_sem=r_send.at[c, source], recv_sem=r_recv.at[c, source],
            device_id={"tile": source}, device_id_type=MESH,
        )

    @pl.loop(1, TILES)
    def _(k):
        slots_of(tile_at(k))
        each_size(lambda n, d: far_to(k, 0, n).start())

    @pl.loop(1, TILES)
    def _(k):
        each_size(lambda n, d: far_to(k, 1, n).start())

    slots_of(tile)
    relay[tile] = send_far[tile]

    def near_up():
        return pltpu.make_async_remote_copy(
            src_ref=send_up, dst_ref=near_ref.at[1], send_sem=near_send.at[0],
            recv_sem=near_recv.at[0], device_id={"band": band_at(1)}, device_id_type=MESH,
        )

    def near_down():
        return pltpu.make_async_remote_copy(
            src_ref=send_down, dst_ref=near_ref.at[2], send_sem=near_send.at[1],
            recv_sem=near_recv.at[1], device_id={"band": band_at(BANDS - 1)}, device_id_type=MESH,
        )

    @pl.when(band < BANDS - 1)
    def _():
        near_up().start()

    @pl.when(band > 0)
    def _():
        near_down().start()

    @pl.loop(1, TILES)
    def _(k):
        note_from(k).wait_recv()

    quarters = []
    for q in range(4):
        quarters.append(
            notes[4 * q, 0:1, :] + notes[4 * q + 1, 0:1, :]
            + notes[4 * q + 2, 0:1, :] + notes[4 * q + 3, 0:1, :]
        )
    label = jnp.concatenate(quarters, axis=1).astype(I32)
    entries = TILES * NC
    filled = label > 0
    label = label - 1
    goes_to, block = label >> 7, label & (BLOCKS - 1)
    is_block = filled & (iota((BLOCKS, entries), 0) == block)
    block_hot = jnp.where(is_block, 1.0, 0.0).astype(BF16)
    owner_hot = jnp.where(
        filled & (iota((TILES, entries), 0) == goes_to), 1.0, 0.0
    ).astype(BF16)
    hits = lax.dot_general(
        block_hot, owner_hot, (((1,), (1,)), ((), ())), preferred_element_type=F32
    )
    taken = jnp.where(hits > 0.0, 1.0, 0.0)
    below = jnp.where(lane < sub, 1.0, 0.0).astype(BF16)
    order = jnp.dot(below, taken.astype(BF16), preferred_element_type=F32)
    spread = jnp.dot(order.astype(BF16), owner_hot, preferred_element_type=F32)
    depth = jnp.sum(jnp.where(is_block, spread, 0.0), axis=0, keepdims=True).astype(I32)
    goal = jnp.where(filled & (depth < DC), goes_to * DC + depth, -1)

    most_far = notes[0, 1:2, :]
    for s in range(1, TILES):
        most_far = jnp.maximum(most_far, notes[s, 1:2, :])
    over_far = jnp.max(
        jnp.where(lane1 == LANES - 1, most_far - jnp.where(edge, NC, NC_MID).astype(F32), 0.0), axis=1, keepdims=True
    )
    load = jnp.sum(taken, axis=0, keepdims=True)
    over_load = jnp.max(load - jnp.where(edge, DC, DC_MID).astype(F32), axis=1, keepdims=True)
    alarm[...] = jnp.broadcast_to(
        jnp.where((over_far > 0.0) | (over_load > 0.0), 1.0, 0.0), (1, LANES)
    )

    def alarm_to(k):
        return pltpu.make_async_remote_copy(
            src_ref=alarm, dst_ref=alarms.at[band], send_sem=alarm_send.at[band_at(k)],
            recv_sem=alarm_recv.at[band], device_id={"band": band_at(k)}, device_id_type=MESH,
        )

    def alarm_from(k):
        source = band_at(BANDS - k)
        return pltpu.make_async_remote_copy(
            src_ref=alarm, dst_ref=alarms.at[source], send_sem=alarm_send.at[source],
            recv_sem=alarm_recv.at[source], device_id={"band": source}, device_id_type=MESH,
        )

    @pl.loop(1, BANDS)
    def _(k):
        alarm_to(k).start()

    alarms[band] = alarm[...]

    @pl.when(band > 0)
    def _():
        note_up().wait_recv()

    @pl.when(band < BANDS - 1)
    def _():
        note_down().wait_recv()

    near_labels = jnp.where(
        lane1 < NEAR,
        note[1:2, :],
        jnp.where(lane1 < 2 * NEAR, notes[TILES, 1:2, :], notes[TILES + 1, 1:2, :]),
    )
    mine = iota((BLOCKS, TILES), 1) == tile
    my_taken = jnp.sum(jnp.where(mine, taken, 0.0), axis=1, keepdims=True)
    my_order = jnp.sum(jnp.where(mine, order, 0.0), axis=1, keepdims=True).astype(I32)
    is_near = (lane < FAR0) & (near_labels.astype(I32) == sub + 1)
    is_far = (lane >= FAR0) & (lane < FAR0 + DC) & (my_taken > 0.0) & (my_order == lane - FAR0)
    put = jnp.where(is_near | is_far, 1.0, 0.0).astype(BF16)
    put2 = jnp.concatenate([put, put], axis=1)

    depth_sub = iota((DC, entries), 0)

    def blocks_of(owner_tile, c):
        hot = jnp.where(depth_sub + owner_tile * DC == goal, 1.0, 0.0).astype(BF16)
        return jnp.dot(
            jnp.concatenate([hot, hot], axis=1), stacked[c], preferred_element_type=F32
        )

    def parcel_to(k, c, d):
        return pltpu.make_async_remote_copy(
            src_ref=parcel.at[tile_at(k), c, pl.ds(0, d)], dst_ref=far_ref.at[tile, c, pl.ds(0, d)],
            send_sem=q_send.at[c, tile_at(k)], recv_sem=q_recv.at[c, tile],
            device_id={"tile": tile_at(k)}, device_id_type=MESH,
        )

    def parcel_from(k, c, d):
        source = tile_at(TILES - k)
        return pltpu.make_async_remote_copy(
            src_ref=parcel.at[source, c, pl.ds(0, d)], dst_ref=far_ref.at[source, c, pl.ds(0, d)],
            send_sem=q_send.at[c, source], recv_sem=q_recv.at[c, source],
            device_id={"tile": source}, device_id_type=MESH,
        )

    for c in range(PIECE):

        @pl.loop(1, TILES)
        def _(k):
            each_size(lambda n, d: far_from(k, c, n).wait_recv())

        high, low = split(relay[:, c].reshape(entries, LANES))
        stacked[c, :entries] = high
        stacked[c, entries:] = low

        @pl.loop(1, TILES)
        def _(k):
            parcel[tile_at(k), c] = blocks_of(tile_at(k), c)
            each_size(lambda n, d: parcel_to(k, c, d).start())

    for c in range(PIECE):
        far_ref[tile, c] = blocks_of(tile, c)

    @pl.when(band > 0)
    def _():
        near_up().wait_recv()

    @pl.when(band < BANDS - 1)
    def _():
        near_down().wait_recv()

    def cells_of(m):
        groups = [
            jnp.concatenate([near_ref[i, m * PIECE + c] for c in range(PIECE)], axis=1)
            for i in range(3)
        ]
        groups.append(jnp.concatenate([far_ref[m, c] for c in range(PIECE)], axis=1))
        total = jnp.dot(
            put2,
            jnp.concatenate(split(jnp.concatenate(groups, axis=0)), axis=0),
            preferred_element_type=F32,
        )
        for c in range(PIECE):
            out_ref[pl.ds(m * PIECE + c, BLOCKS, stride=CELLS), :] = total[
                :, c * LANES : (c + 1) * LANES
            ]

    cells_of(tile)

    @pl.loop(1, TILES)
    def _(k):
        for c in range(PIECE):
            each_size(lambda n, d: parcel_from(k, c, d).wait_recv())
        cells_of(tile_at(TILES - k))

    @pl.loop(1, BANDS)
    def _(k):
        alarm_from(k).wait_recv()

    flag_ref[0] = jnp.max(alarms[...]).astype(I32)

    @pl.when(band > 0)
    def _():
        note_down().wait_send()
        near_down().wait_send()

    @pl.when(band < BANDS - 1)
    def _():
        note_up().wait_send()
        near_up().wait_send()

    @pl.loop(1, BANDS)
    def _(k):
        alarm_to(k).wait_send()

    @pl.loop(1, TILES)
    def _(k):
        note_to(k).wait_send()
        for c in range(PIECE):
            each_size(lambda n, d: far_to(k, c, n).wait_send())
            each_size(lambda n, d: parcel_to(k, c, d).wait_send())


def exchange(patches, pair_patch, pair_atm, numerators, counts):
    vmem = pl.BlockSpec(memory_space=pltpu.VMEM)
    smem = pl.BlockSpec(memory_space=pltpu.SMEM)
    anywhere = pl.BlockSpec(memory_space=pl.ANY)
    dma = pltpu.SemaphoreType.DMA
    return pl.pallas_call(
        exchange_kernel,
        out_shape=(
            jax.ShapeDtypeStruct((BLOCKS * CELLS, LANES), F32),
            jax.ShapeDtypeStruct((1,), I32),
        ),
        in_specs=[smem, anywhere, anywhere, anywhere, anywhere],
        out_specs=(vmem, smem),
        scratch_shapes=[
            pltpu.SMEM((PAIRS,), I32),
            pltpu.VMEM((1, PAIRS), I32),
            pltpu.VMEM((PAIRS, CELLS, LANES), I32),
            pltpu.VMEM((PAIRS // 2, LANES, LANES), BF16),
            pltpu.VMEM((CELLS * PAIRS, LANES), F32),
            pltpu.VMEM((TILES, PIECE, NC, LANES), F32),
            pltpu.VMEM((CELLS, NEAR, LANES), F32),
            pltpu.VMEM((CELLS, NEAR, LANES), F32),
            pltpu.VMEM((TILES, PIECE, NC, LANES), F32),
            pltpu.VMEM((PIECE, 2 * TILES * NC, LANES), BF16),
            pltpu.VMEM((TILES, PIECE, DC, LANES), F32),
            pltpu.VMEM((TILES, PIECE, DC, LANES), F32),
            pltpu.VMEM((3, CELLS, NEAR, LANES), F32),
            pltpu.VMEM((2, LANES), F32),
            pltpu.VMEM((TILES + 2, 2, LANES), F32),
            pltpu.VMEM((1, LANES), F32),
            pltpu.VMEM((BANDS, 1, LANES), F32),
            dma((7,)),
            dma((TILES + 2,)), dma((TILES + 2,)),
            dma((PIECE, TILES)), dma((PIECE, TILES)),
            dma((PIECE, TILES)), dma((PIECE, TILES)),
            dma((2,)), dma((2,)),
            dma((BANDS,)), dma((BANDS,)),
        ],
        compiler_params=pltpu.CompilerParams(
            collective_id=0, has_side_effects=True, vmem_limit_bytes=40 * 2**20
        ),
        name="exchange",
    )(
        counts,
        pair_patch,
        pair_atm.reshape(1, PAIRS),
        numerators.transpose(0, 2, 1),
        patches.reshape(-1, LANES, LANES),
    )


def put_kernel(total_ref, out_ref, sem):
    parts = sem.shape[0]
    rows = total_ref.shape[0] // parts
    copies = [
        pltpu.make_async_copy(
            total_ref.at[pl.ds(i * rows, rows)], out_ref.at[pl.ds(i * rows, rows)], sem.at[i]
        )
        for i in range(parts)
    ]
    for copy in copies:
        copy.start()
    for copy in copies:
        copy.wait()


def put(total):
    return pl.pallas_call(
        put_kernel,
        out_shape=jax.ShapeDtypeStruct(total.shape, F32),
        in_specs=[pl.BlockSpec(memory_space=pltpu.VMEM)],
        out_specs=pl.BlockSpec(memory_space=pl.ANY),
        scratch_shapes=[pltpu.SemaphoreType.DMA((4,))],
        compiler_params=pltpu.CompilerParams(vmem_limit_bytes=8 * 2**20),
        name="put",
    )(total)


def shifted(value, axis, steps):
    count = lax.axis_size(axis)
    first, last = (max(0, -steps), min(count, count - steps))
    return lax.ppermute(value, axis, [(source, source + steps) for source in range(first, last)])


def slot_ranks(owners, blocks_local, live_pairs):
    position = jnp.arange(owners.shape[0])
    earlier = position[None, :] < position[:, None]
    both_live = live_pairs[None, :] & live_pairs[:, None]
    same_owner = (owners[:, None] == owners[None, :]) & both_live
    same_block = same_owner & (blocks_local[:, None] == blocks_local[None, :])
    leading = jnp.logical_not(jnp.any(same_block & earlier, axis=1))
    leader_rank = jnp.sum((same_owner & earlier & leading[None, :]).astype(jnp.int32), axis=1)
    first_match = same_block & leading[None, :]
    return jnp.sum(jnp.where(first_match, leader_rank[None, :], 0), axis=1)


def pack(flattened, rows_index, selected, blocks_local, rows_total):
    onehot = (rows_index[None, :] == jnp.arange(rows_total)[:, None]) & selected[None, :]
    payload = jnp.dot(onehot.astype(jnp.float32), flattened, precision=lax.Precision.HIGHEST)
    labels = jnp.max(jnp.where(onehot, blocks_local[None, :], -1), axis=1)
    return (payload, labels)


def unpack(payload, labels, blocks_owned):
    onehot = (labels[None, :] == jnp.arange(blocks_owned)[:, None]).astype(jnp.float32)
    return jnp.dot(onehot, payload, precision=lax.Precision.HIGHEST)


def along_band(parcel, offset_by):
    return shifted((parcel[0], parcel[1]), "band", offset_by)


def long_route(patches, pair_patch, pair_atm, numerators, counts):
    pairs_here, patch_rows, cell_rows = numerators.shape
    flux_width = patches.shape[1]
    blocks_owned = CELLS_DEV // cell_rows
    capacity = pairs_here // 4
    grouped = patches.reshape(-1, patch_rows, flux_width)
    live_pairs = jnp.arange(pairs_here) < counts[0]
    weight = (numerators.astype(jnp.float32) * SCALE).astype(jnp.bfloat16)
    chosen = grouped[pair_patch]
    partial_value = jnp.einsum("jpa,jpf->jaf", weight, chosen, preferred_element_type=jnp.float32)
    flattened = partial_value.reshape(pairs_here, cell_rows * flux_width)
    owners = pair_atm // blocks_owned
    blocks_local = pair_atm % blocks_owned
    slot_rank = slot_ranks(owners, blocks_local, live_pairs)
    bucket_size = capacity // 2
    tile_count = lax.axis_size("tile")
    band_now = lax.axis_index("band")
    tile_now = lax.axis_index("tile")
    owner_band = owners // tile_count
    owner_tile = owners % tile_count
    in_band = live_pairs & (owner_band == band_now)
    rows_index = jnp.where(in_band, owner_tile * bucket_size + slot_rank, -1)
    payload, labels = pack(flattened, rows_index, in_band, blocks_local, tile_count * bucket_size)

    def bucket(target):
        addressed = live_pairs & (owners == target)
        target_rows = jnp.where(addressed, slot_rank, -1)
        return pack(flattened, target_rows, addressed, blocks_local, bucket_size)

    upper_index = (band_now + 1) * tile_count + tile_now
    lower_index = (band_now - 1) * tile_count + tile_now
    from_below = along_band(bucket(upper_index), 1)
    from_above = along_band(bucket(lower_index), -1)
    band_payload = jnp.concatenate([from_below[0], from_above[0]], axis=0)
    band_labels = jnp.concatenate([from_below[1], from_above[1]], axis=0)
    payload, labels = (
        lax.all_to_all(
            payload.reshape(tile_count, bucket_size, -1),
            "tile",
            split_axis=0,
            concat_axis=0,
            tiled=True,
        ),
        lax.all_to_all(
            labels.reshape(tile_count, bucket_size), "tile", split_axis=0, concat_axis=0, tiled=True
        ),
    )
    payload = jnp.concatenate([payload.reshape(tile_count * bucket_size, -1), band_payload], axis=0)
    labels = jnp.concatenate([labels.reshape(-1), band_labels], axis=0)
    summed = unpack(payload, labels, blocks_owned)
    return summed.reshape(blocks_owned * cell_rows, flux_width)


def per_device(patches, pair_patch, pair_atm, numerators, counts):
    total, flag = exchange(patches, pair_patch, pair_atm, numerators, counts)
    return lax.cond(
        flag[0] == 0,
        lambda: put(total),
        lambda: long_route(patches, pair_patch, pair_atm, numerators, counts),
    )


def solution(mesh):
    placed = (
        P(("band", "tile"), None),
        P(("band", "tile")),
        P(("band", "tile")),
        P(("band", "tile"), None, None),
        P(("band", "tile")),
    )
    return jax.shard_map(
        per_device, mesh=mesh, in_specs=placed, out_specs=P(("band", "tile"), None), check_vma=False
    )
```

```python
import functools

import jax
import jax.numpy as jnp
from jax import lax
from jax.experimental import pallas as pl
from jax.experimental.pallas import tpu as pltpu
from jax.sharding import PartitionSpec as P

CELLS_DEV = 4096
SCALE = 2.0 ** (-27)

TILES = 16
BANDS = 8
PAIRS = 128
CELLS = 32
LANES = 128
BLOCKS = 128
NEAR = 16
FAR0 = 3 * NEAR
SLOTS = 128 + 8
NONE = 128
GROUP = 4
NC = 32
DC = 80
NC_MID, DC_MID = 16, 72
PIECE = CELLS // TILES
MESH = pl.DeviceIdType.MESH
F32, BF16, I32 = jnp.float32, jnp.bfloat16, jnp.int32


def iota(shape, axis):
    return lax.broadcasted_iota(I32, shape, axis)


def split(value):
    high = value.astype(BF16)
    return high, (value - high.astype(F32)).astype(BF16)


def exchange_kernel(
    counts_ref, patch_hbm, atm_hbm, num_hbm, patches_hbm,
    all_ref, index_ref, flag_ref,
    patch_ref, atm_ref, num_v, pat_v, table, table_s, part, send_far, send_up, send_down,
    relay, stacked, parcel, note, notes, alarm, alarms,
    in_sem, table_sem, note_send, note_recv, r_send, r_recv, q_send, q_recv,
    near_send, near_recv, alarm_send, alarm_recv,
):
    band, tile = lax.axis_index("band"), lax.axis_index("tile")
    edge = (band == 0) | (band == BANDS - 1)
    chunks = in_sem.shape[0] - 3
    rows = PAIRS // chunks

    def tile_at(k):
        return lax.rem(tile + k, TILES)

    def band_at(k):
        return lax.rem(band + k, BANDS)

    def each_size(body):
        @pl.when(edge)
        def _():
            body(NC, DC)

        @pl.when(jnp.logical_not(edge))
        def _():
            body(NC_MID, DC_MID)

    atm_copy = pltpu.make_async_copy(atm_hbm, atm_ref, in_sem.at[chunks + 1])
    atm_copy.start()
    patch_copy = pltpu.make_async_copy(patch_hbm, patch_ref, in_sem.at[chunks + 2])
    patch_copy.start()
    pat_copy = pltpu.make_async_copy(patches_hbm, pat_v, in_sem.at[chunks])
    pat_copy.start()
    num_copies = [
        pltpu.make_async_copy(
            num_hbm.at[pl.ds(i * rows, rows)], num_v.at[pl.ds(i * rows, rows)], in_sem.at[i]
        )
        for i in range(chunks)
    ]
    for copy in num_copies:
        copy.start()

    barrier = pltpu.get_barrier_semaphore()

    @pl.loop(1, TILES)
    def _(k):
        pl.semaphore_signal(barrier, inc=1, device_id={"tile": tile_at(k)}, device_id_type=MESH)

    @pl.loop(1, BANDS)
    def _(k):
        pl.semaphore_signal(barrier, inc=1, device_id={"band": band_at(k)}, device_id_type=MESH)

    lane, sub = iota((PAIRS, LANES), 1), iota((PAIRS, LANES), 0)
    lane1 = iota((1, LANES), 1)

    def column(row):
        return jnp.sum(jnp.where(lane == sub, row, 0.0), axis=1, keepdims=True)

    atm_copy.wait()
    atm = atm_ref[...]
    live = lane1 < counts_ref[0]
    owner = atm >> 7
    me = band * TILES + tile
    base = jnp.where(
        owner == me,
        0,
        jnp.where(owner == me + TILES, NEAR, jnp.where(owner == me - TILES, 2 * NEAR, FAR0)),
    ).astype(F32)
    key = jnp.where(live, atm, -1).astype(F32)
    key_c, base_c = column(key), column(base)
    same = (key_c == key) & (key >= 0.0)
    earlier = jnp.sum(jnp.where(same & (sub < lane), 1.0, 0.0), axis=0, keepdims=True)
    first = jnp.where(live & (earlier == 0.0), 1.0, 0.0)
    first_c = column(first)
    ahead = (first_c > 0.0) & (base_c == base) & (key_c < key)
    rank = jnp.sum(jnp.where(ahead, 1.0, 0.0), axis=0, keepdims=True)
    slot = jnp.where(live, base + rank, -1.0)
    slot_c = column(slot).astype(I32)
    leads = first_c > 0.0
    later = jnp.sum(jnp.where(same & (sub > lane), 1.0, 0.0), axis=0, keepdims=True)
    last_c = column(jnp.where(live & (later == 0.0), 1.0, 0.0))
    turn = jnp.where(live, slot, 2.0 * PAIRS)
    turn_c = column(turn)
    before = (turn_c < turn) | ((turn_c == turn) & (sub < lane))
    place_c = column(jnp.sum(jnp.where(before, 1.0, 0.0), axis=0, keepdims=True)).astype(I32)
    at = place_c == lane
    table[0:1, :] = jnp.sum(jnp.where(at, sub, 0), axis=0, keepdims=True)
    joins_c = column(earlier).astype(I32)
    table[1:2, :] = jnp.sum(jnp.where(at & (joins_c > 0), 1, 0), axis=0, keepdims=True)
    ends = (last_c > 0.0) & (slot_c == lane)
    table[2:3, :] = PAIRS + jnp.sum(jnp.where(ends, place_c - PAIRS, 0), axis=0, keepdims=True)
    table_copy = pltpu.make_async_copy(table, table_s, table_sem)
    table_copy.start()
    key_i = key_c.astype(I32)
    far_lane = slot_c - FAR0 + NC * lax.rem(tile, 4)
    in_far = leads & (slot_c >= FAR0) & (slot_c < FAR0 + NC)
    far_label = (key_i - band * (TILES * BLOCKS) + 1).astype(F32)
    far_row = jnp.sum(jnp.where(in_far & (far_lane == lane), far_label, 0.0), axis=0, keepdims=True)
    in_near = leads & (slot_c < FAR0) & (slot_c == lane)
    near_label = ((key_i & (BLOCKS - 1)) + 1).astype(F32)
    near_row = jnp.sum(jnp.where(in_near, near_label, 0.0), axis=0, keepdims=True)
    n_far = jnp.sum(jnp.where(base == FAR0, first, 0.0), axis=1, keepdims=True)
    note[0:1, :] = far_row
    note[1:2, :] = jnp.where(lane1 == LANES - 1, n_far, near_row)

    @pl.when(band == 0)
    def _():
        notes[TILES] = jnp.zeros((2, LANES), F32)

    @pl.when(band == BANDS - 1)
    def _():
        notes[TILES + 1] = jnp.zeros((2, LANES), F32)

    @pl.when(jnp.logical_not(edge))
    def _():
        relay[:, :, NC_MID:] = jnp.zeros((TILES, PIECE, NC - NC_MID, LANES), F32)

    all_ref[:, NONE:] = jnp.zeros((CELLS, SLOTS - NONE, LANES), F32)
    part[PAIRS] = jnp.zeros((CELLS, LANES), F32)

    patch_copy.wait()
    table_copy.wait()
    pat_copy.wait()
    for copy in num_copies:
        copy.wait()

    def add_pair(i, total):
        g = table_s[0, i]
        weight = (num_v[g].astype(F32) * SCALE).astype(BF16)
        product = jnp.dot(weight, pat_v[patch_ref[g]], preferred_element_type=F32)
        total = jnp.where(table_s[1, i] > 0, total, 0.0) + product
        part[i] = total
        return total

    lax.fori_loop(0, PAIRS, add_pair, jnp.zeros((CELLS, LANES), F32), unroll=8)

    self_rows = all_ref.reshape(CELLS * SLOTS, LANES)
    up_rows = send_up.reshape(CELLS * NEAR, LANES)
    down_rows = send_down.reshape(CELLS * NEAR, LANES)

    @pl.loop(0, NC, unroll=4)
    def _(j):
        send_far[pl.ds(j, CELLS, stride=NC), :] = part[table_s[2, FAR0 + j]]

    pl.semaphore_wait(barrier, TILES + BANDS - 2)

    def note_to(k):
        return pltpu.make_async_remote_copy(
            src_ref=note, dst_ref=notes.at[tile], send_sem=note_send.at[tile_at(k)],
            recv_sem=note_recv.at[tile], device_id={"tile": tile_at(k)}, device_id_type=MESH,
        )

    def note_from(k):
        source = tile_at(TILES - k)
        return pltpu.make_async_remote_copy(
            src_ref=note, dst_ref=notes.at[source], send_sem=note_send.at[source],
            recv_sem=note_recv.at[source], device_id={"tile": source}, device_id_type=MESH,
        )

    def note_up():
        return pltpu.make_async_remote_copy(
            src_ref=note, dst_ref=notes.at[TILES], send_sem=note_send.at[TILES],
            recv_sem=note_recv.at[TILES], device_id={"band": band_at(1)}, device_id_type=MESH,
        )

    def note_down():
        return pltpu.make_async_remote_copy(
            src_ref=note, dst_ref=notes.at[TILES + 1], send_sem=note_send.at[TILES + 1],
            recv_sem=note_recv.at[TILES + 1], device_id={"band": band_at(BANDS - 1)},
            device_id_type=MESH,
        )

    @pl.loop(1, TILES)
    def _(k):
        note_to(k).start()

    @pl.when(band < BANDS - 1)
    def _():
        note_up().start()

    @pl.when(band > 0)
    def _():
        note_down().start()

    notes[tile] = note[...]

    def far_to(k, c, n):
        return pltpu.make_async_remote_copy(
            src_ref=send_far.at[pl.ds((tile_at(k) * PIECE + c) * NC, n)], dst_ref=relay.at[tile, c, pl.ds(0, n)],
            send_sem=r_send.at[c, tile_at(k)], recv_sem=r_recv.at[c, tile],
            device_id={"tile": tile_at(k)}, device_id_type=MESH,
        )

    def far_from(k, c, n):
        source = tile_at(TILES - k)
        return pltpu.make_async_remote_copy(
            src_ref=send_far.at[pl.ds((source * PIECE + c) * NC, n)], dst_ref=relay.at[source, c, pl.ds(0, n)],
            send_sem=r_send.at[c, source], recv_sem=r_recv.at[c, source],
            device_id={"tile": source}, device_id_type=MESH,
        )

    for c in range(PIECE):

        @pl.loop(1, TILES)
        def _(k):
            each_size(lambda n, d: far_to(k, c, n).start())

    for c in range(PIECE):
        relay[tile, c] = send_far[pl.ds((tile * PIECE + c) * NC, NC), :]

    @pl.loop(0, NEAR, unroll=4)
    def _(j):
        up_rows[pl.ds(j, CELLS, stride=NEAR), :] = part[table_s[2, NEAR + j]]
        down_rows[pl.ds(j, CELLS, stride=NEAR), :] = part[table_s[2, 2 * NEAR + j]]

    def near_up():
        return pltpu.make_async_remote_copy(
            src_ref=send_up, dst_ref=all_ref.at[:, pl.ds(NEAR, NEAR)], send_sem=near_send.at[0],
            recv_sem=near_recv.at[0], device_id={"band": band_at(1)}, device_id_type=MESH,
        )

    def near_down():
        return pltpu.make_async_remote_copy(
            src_ref=send_down, dst_ref=all_ref.at[:, pl.ds(2 * NEAR, NEAR)], send_sem=near_send.at[1],
            recv_sem=near_recv.at[1], device_id={"band": band_at(BANDS - 1)}, device_id_type=MESH,
        )

    @pl.when(band < BANDS - 1)
    def _():
        near_up().start()

    @pl.when(band > 0)
    def _():
        near_down().start()

    @pl.loop(0, NEAR, unroll=4)
    def _(j):
        self_rows[pl.ds(j, CELLS, stride=SLOTS), :] = part[table_s[2, j]]

    @pl.loop(1, TILES)
    def _(k):
        note_from(k).wait_recv()

    quarters = []
    for q in range(4):
        quarters.append(
            notes[4 * q, 0:1, :] + notes[4 * q + 1, 0:1, :]
            + notes[4 * q + 2, 0:1, :] + notes[4 * q + 3, 0:1, :]
        )
    label = jnp.concatenate(quarters, axis=1).astype(I32)
    entries = TILES * NC
    filled = label > 0
    label = label - 1
    goes_to, block = label >> 7, label & (BLOCKS - 1)
    is_block = filled & (iota((BLOCKS, entries), 0) == block)
    block_hot = jnp.where(is_block, 1.0, 0.0).astype(BF16)
    owner_hot = jnp.where(
        filled & (iota((TILES, entries), 0) == goes_to), 1.0, 0.0
    ).astype(BF16)
    hits = lax.dot_general(
        block_hot, owner_hot, (((1,), (1,)), ((), ())), preferred_element_type=F32
    )
    taken = jnp.where(hits > 0.0, 1.0, 0.0)
    below = jnp.where(lane < sub, 1.0, 0.0).astype(BF16)
    order = jnp.dot(below, taken.astype(BF16), preferred_element_type=F32)
    spread = jnp.dot(order.astype(BF16), owner_hot, preferred_element_type=F32)
    depth = jnp.sum(jnp.where(is_block, spread, 0.0), axis=0, keepdims=True).astype(I32)
    goal = jnp.where(filled & (depth < DC), goes_to * DC + depth, -1)

    most_far = notes[0, 1:2, :]
    for s in range(1, TILES):
        most_far = jnp.maximum(most_far, notes[s, 1:2, :])
    over_far = jnp.max(
        jnp.where(lane1 == LANES - 1, most_far - jnp.where(edge, NC, NC_MID).astype(F32), 0.0), axis=1, keepdims=True
    )
    load = jnp.sum(taken, axis=0, keepdims=True)
    over_load = jnp.max(load - jnp.where(edge, DC, DC_MID).astype(F32), axis=1, keepdims=True)
    alarm[...] = jnp.broadcast_to(
        jnp.where((over_far > 0.0) | (over_load > 0.0), 1.0, 0.0), (1, LANES)
    )

    def alarm_to(k):
        return pltpu.make_async_remote_copy(
            src_ref=alarm, dst_ref=alarms.at[band], send_sem=alarm_send.at[band_at(k)],
            recv_sem=alarm_recv.at[band], device_id={"band": band_at(k)}, device_id_type=MESH,
        )

    def alarm_from(k):
        source = band_at(BANDS - k)
        return pltpu.make_async_remote_copy(
            src_ref=alarm, dst_ref=alarms.at[source], send_sem=alarm_send.at[source],
            recv_sem=alarm_recv.at[source], device_id={"band": source}, device_id_type=MESH,
        )

    @pl.loop(1, BANDS)
    def _(k):
        alarm_to(k).start()

    alarms[band] = alarm[...]

    @pl.when(band > 0)
    def _():
        note_up().wait_recv()

    @pl.when(band < BANDS - 1)
    def _():
        note_down().wait_recv()

    near_labels = jnp.where(
        lane1 < NEAR,
        note[1:2, :],
        jnp.where(lane1 < 2 * NEAR, notes[TILES, 1:2, :], notes[TILES + 1, 1:2, :]),
    )
    here = column(near_labels).astype(I32) == lane + 1
    for i in range(3):
        found = here & (sub >= i * NEAR) & (sub < (i + 1) * NEAR)
        index_ref[i : i + 1, :] = NONE + jnp.sum(
            jnp.where(found, sub - NONE, 0), axis=0, keepdims=True
        )
    mine = iota((BLOCKS, TILES), 1) == tile
    my_row = jnp.sum(
        jnp.where(mine & (taken > 0.0), order + FAR0 - NONE, 0.0), axis=1, keepdims=True
    )
    index_ref[3:4, :] = NONE + jnp.sum(
        jnp.where(lane == sub, my_row, 0.0), axis=0, keepdims=True
    ).astype(I32)

    depth_sub = iota((GROUP * DC, entries), 0)

    def blocks_of(group, c):
        hot = jnp.where(depth_sub + group * (GROUP * DC) == goal, 1.0, 0.0).astype(BF16)
        return jnp.dot(
            jnp.concatenate([hot, hot], axis=1), stacked[c], preferred_element_type=F32
        ).reshape(GROUP, DC, LANES)

    def parcel_to(target, c, d):
        return pltpu.make_async_remote_copy(
            src_ref=parcel.at[target, c, pl.ds(0, d)],
            dst_ref=all_ref.at[tile * PIECE + c, pl.ds(FAR0, d)],
            send_sem=q_send.at[c, target], recv_sem=q_recv.at[c, tile],
            device_id={"tile": target}, device_id_type=MESH,
        )

    def parcel_from(source, c, d):
        return pltpu.make_async_remote_copy(
            src_ref=parcel.at[source, c, pl.ds(0, d)],
            dst_ref=all_ref.at[source * PIECE + c, pl.ds(FAR0, d)],
            send_sem=q_send.at[c, source], recv_sem=q_recv.at[c, source],
            device_id={"tile": source}, device_id_type=MESH,
        )

    for c in range(PIECE):

        @pl.loop(1, TILES)
        def _(k):
            each_size(lambda n, d: far_from(k, c, n).wait_recv())

        high, low = split(relay[:, c].reshape(entries, LANES))
        stacked[c, :entries] = high
        stacked[c, entries:] = low

        @pl.loop(1, GROUP + 1)
        def _(q):
            group = lax.rem(tile // GROUP + q, GROUP)
            parcel[pl.ds(group * GROUP, GROUP), c] = blocks_of(group, c)

            @pl.loop(0, GROUP)
            def _(k):
                target = group * GROUP + lax.rem(tile + k, GROUP)

                @pl.when(target != tile)
                def _():
                    each_size(lambda n, d: parcel_to(target, c, d).start())

    for c in range(PIECE):
        all_ref[tile * PIECE + c, FAR0:NONE] = parcel[tile, c]

    @pl.loop(1, BANDS)
    def _(k):
        alarm_from(k).wait_recv()

    flag_ref[0] = jnp.max(alarms[...]).astype(I32)

    @pl.when(band > 0)
    def _():
        near_up().wait_recv()
        note_down().wait_send()
        near_down().wait_send()

    @pl.when(band < BANDS - 1)
    def _():
        near_down().wait_recv()
        note_up().wait_send()
        near_up().wait_send()

    @pl.loop(1, BANDS)
    def _(k):
        alarm_to(k).wait_send()

    @pl.loop(1, TILES)
    def _(k):
        note_to(k).wait_send()
        for c in range(PIECE):
            each_size(lambda n, d: far_to(k, c, n).wait_send())
            each_size(lambda n, d: parcel_to(tile_at(k), c, d).wait_send())
            each_size(lambda n, d: parcel_from(tile_at(k), c, d).wait_recv())


def exchange(patches, pair_patch, pair_atm, numerators, counts):
    vmem = pl.BlockSpec(memory_space=pltpu.VMEM)
    smem = pl.BlockSpec(memory_space=pltpu.SMEM)
    anywhere = pl.BlockSpec(memory_space=pl.ANY)
    dma = pltpu.SemaphoreType.DMA
    return pl.pallas_call(
        exchange_kernel,
        out_shape=(
            jax.ShapeDtypeStruct((CELLS, SLOTS, LANES), F32),
            jax.ShapeDtypeStruct((4, BLOCKS), I32),
            jax.ShapeDtypeStruct((1,), I32),
        ),
        in_specs=[smem, anywhere, anywhere, anywhere, anywhere],
        out_specs=(vmem, vmem, smem),
        scratch_shapes=[
            pltpu.SMEM((PAIRS,), I32),
            pltpu.VMEM((1, PAIRS), I32),
            pltpu.VMEM((PAIRS, CELLS, LANES), I32),
            pltpu.VMEM((PAIRS // 2, LANES, LANES), BF16),
            pltpu.VMEM((8, PAIRS), I32),
            pltpu.SMEM((8, PAIRS), I32),
            pltpu.VMEM((PAIRS + 1, CELLS, LANES), F32),
            pltpu.VMEM((CELLS * NC, LANES), F32),
            pltpu.VMEM((CELLS, NEAR, LANES), F32),
            pltpu.VMEM((CELLS, NEAR, LANES), F32),
            pltpu.VMEM((TILES, PIECE, NC, LANES), F32),
            pltpu.VMEM((PIECE, 2 * TILES * NC, LANES), BF16),
            pltpu.VMEM((TILES, PIECE, DC, LANES), F32),
            pltpu.VMEM((2, LANES), F32),
            pltpu.VMEM((TILES + 2, 2, LANES), F32),
            pltpu.VMEM((1, LANES), F32),
            pltpu.VMEM((BANDS, 1, LANES), F32),
            dma((7,)), dma,
            dma((TILES + 2,)), dma((TILES + 2,)),
            dma((PIECE, TILES)), dma((PIECE, TILES)),
            dma((PIECE, TILES)), dma((PIECE, TILES)),
            dma((2,)), dma((2,)),
            dma((BANDS,)), dma((BANDS,)),
        ],
        compiler_params=pltpu.CompilerParams(
            collective_id=0, has_side_effects=True, vmem_limit_bytes=24 * 2**20
        ),
        name="exchange",
    )(
        counts,
        pair_patch,
        pair_atm.reshape(1, PAIRS),
        numerators.transpose(0, 2, 1),
        patches.reshape(-1, LANES, LANES),
    )


def place_kernel(index_ref, all_ref, out_ref, total, sem):
    parts = sem.shape[0]
    blocks = BLOCKS // parts
    copies = []
    for i in range(parts):

        @pl.loop(i * blocks, (i + 1) * blocks, unroll=4)
        def _(a):
            rows = [
                all_ref[pl.ds(index_ref[r, a], CELLS, stride=SLOTS), :] for r in range(4)
            ]
            total[pl.ds(a * CELLS, CELLS), :] = (rows[0] + rows[1]) + (rows[2] + rows[3])

        here = pl.ds(i * blocks * CELLS, blocks * CELLS)
        copies.append(pltpu.make_async_copy(total.at[here], out_ref.at[here], sem.at[i]))
        copies[-1].start()
    for copy in copies:
        copy.wait()


def place(everything, index):
    return pl.pallas_call(
        place_kernel,
        out_shape=jax.ShapeDtypeStruct((BLOCKS * CELLS, LANES), F32),
        in_specs=[
            pl.BlockSpec(memory_space=pltpu.SMEM),
            pl.BlockSpec(memory_space=pltpu.VMEM),
        ],
        out_specs=pl.BlockSpec(memory_space=pl.ANY),
        scratch_shapes=[
            pltpu.VMEM((BLOCKS * CELLS, LANES), F32),
            pltpu.SemaphoreType.DMA((8,)),
        ],
        compiler_params=pltpu.CompilerParams(vmem_limit_bytes=16 * 2**20),
        name="place",
    )(index, everything.reshape(CELLS * SLOTS, LANES))


def shifted(value, axis, steps):
    count = lax.axis_size(axis)
    first, last = (max(0, -steps), min(count, count - steps))
    return lax.ppermute(value, axis, [(source, source + steps) for source in range(first, last)])


def slot_ranks(owners, blocks_local, live_pairs):
    position = jnp.arange(owners.shape[0])
    earlier = position[None, :] < position[:, None]
    both_live = live_pairs[None, :] & live_pairs[:, None]
    same_owner = (owners[:, None] == owners[None, :]) & both_live
    same_block = same_owner & (blocks_local[:, None] == blocks_local[None, :])
    leading = jnp.logical_not(jnp.any(same_block & earlier, axis=1))
    leader_rank = jnp.sum((same_owner & earlier & leading[None, :]).astype(jnp.int32), axis=1)
    first_match = same_block & leading[None, :]
    return jnp.sum(jnp.where(first_match, leader_rank[None, :], 0), axis=1)


def pack(flattened, rows_index, selected, blocks_local, rows_total):
    onehot = (rows_index[None, :] == jnp.arange(rows_total)[:, None]) & selected[None, :]
    payload = jnp.dot(onehot.astype(jnp.float32), flattened, precision=lax.Precision.HIGHEST)
    labels = jnp.max(jnp.where(onehot, blocks_local[None, :], -1), axis=1)
    return (payload, labels)


def unpack(payload, labels, blocks_owned):
    onehot = (labels[None, :] == jnp.arange(blocks_owned)[:, None]).astype(jnp.float32)
    return jnp.dot(onehot, payload, precision=lax.Precision.HIGHEST)


def along_band(parcel, offset_by):
    return shifted((parcel[0], parcel[1]), "band", offset_by)


def long_route(patches, pair_patch, pair_atm, numerators, counts):
    pairs_here, patch_rows, cell_rows = numerators.shape
    flux_width = patches.shape[1]
    blocks_owned = CELLS_DEV // cell_rows
    capacity = pairs_here // 4
    grouped = patches.reshape(-1, patch_rows, flux_width)
    live_pairs = jnp.arange(pairs_here) < counts[0]
    weight = (numerators.astype(jnp.float32) * SCALE).astype(jnp.bfloat16)
    chosen = grouped[pair_patch]
    partial_value = jnp.einsum("jpa,jpf->jaf", weight, chosen, preferred_element_type=jnp.float32)
    flattened = partial_value.reshape(pairs_here, cell_rows * flux_width)
    owners = pair_atm // blocks_owned
    blocks_local = pair_atm % blocks_owned
    slot_rank = slot_ranks(owners, blocks_local, live_pairs)
    bucket_size = capacity // 2
    tile_count = lax.axis_size("tile")
    band_now = lax.axis_index("band")
    tile_now = lax.axis_index("tile")
    owner_band = owners // tile_count
    owner_tile = owners % tile_count
    in_band = live_pairs & (owner_band == band_now)
    rows_index = jnp.where(in_band, owner_tile * bucket_size + slot_rank, -1)
    payload, labels = pack(flattened, rows_index, in_band, blocks_local, tile_count * bucket_size)

    def bucket(target):
        addressed = live_pairs & (owners == target)
        target_rows = jnp.where(addressed, slot_rank, -1)
        return pack(flattened, target_rows, addressed, blocks_local, bucket_size)

    upper_index = (band_now + 1) * tile_count + tile_now
    lower_index = (band_now - 1) * tile_count + tile_now
    from_below = along_band(bucket(upper_index), 1)
    from_above = along_band(bucket(lower_index), -1)
    band_payload = jnp.concatenate([from_below[0], from_above[0]], axis=0)
    band_labels = jnp.concatenate([from_below[1], from_above[1]], axis=0)
    payload, labels = (
        lax.all_to_all(
            payload.reshape(tile_count, bucket_size, -1),
            "tile",
            split_axis=0,
            concat_axis=0,
            tiled=True,
        ),
        lax.all_to_all(
            labels.reshape(tile_count, bucket_size), "tile", split_axis=0, concat_axis=0, tiled=True
        ),
    )
    payload = jnp.concatenate([payload.reshape(tile_count * bucket_size, -1), band_payload], axis=0)
    labels = jnp.concatenate([labels.reshape(-1), band_labels], axis=0)
    summed = unpack(payload, labels, blocks_owned)
    return summed.reshape(blocks_owned * cell_rows, flux_width)


def per_device(patches, pair_patch, pair_atm, numerators, counts):
    everything, index, flag = exchange(patches, pair_patch, pair_atm, numerators, counts)
    return lax.cond(
        flag[0] == 0,
        lambda: place(everything, index),
        lambda: long_route(patches, pair_patch, pair_atm, numerators, counts),
    )


def solution(mesh):
    placed = (
        P(("band", "tile"), None),
        P(("band", "tile")),
        P(("band", "tile")),
        P(("band", "tile"), None, None),
        P(("band", "tile")),
    )
    return jax.shard_map(
        per_device, mesh=mesh, in_specs=placed, out_specs=P(("band", "tile"), None), check_vma=False
    )
```

```python
import functools

import jax
import jax.numpy as jnp
from jax import lax
from jax.experimental import pallas as pl
from jax.experimental.pallas import tpu as pltpu
from jax.sharding import PartitionSpec as P

CELLS_DEV = 4096
SCALE = 2.0 ** (-27)

TILES = 16
BANDS = 8
PAIRS = 128
CELLS = 32
LANES = 128
BLOCKS = 128
NEAR = 16
FAR0 = 3 * NEAR
GROUP = 4
NC = 32
DC = 80
NC_MID, DC_MID = 16, 72
NEAR_STEP, NC_STEP, DC_STEP = NEAR + 4, NC + 4, DC + 4
PIECE = CELLS // TILES
MESH = pl.DeviceIdType.MESH
F32, BF16, I32 = jnp.float32, jnp.bfloat16, jnp.int32


def iota(shape, axis):
    return lax.broadcasted_iota(I32, shape, axis)


def split(value):
    high = value.astype(BF16)
    return high, (value - high.astype(F32)).astype(BF16)


def exchange_kernel(
    counts_ref, patch_hbm, atm_hbm, num_hbm, patches_hbm,
    far_ref, near_ref, index_s, flag_ref,
    index_ref, patch_ref, atm_ref, num_v, pat_v, table, table_s, part, send_far, send_up, send_down,
    relay, stacked, parcel, note, notes, alarm, alarms,
    in_sem, table_sem, note_send, note_recv, r_send, r_recv, q_send, q_recv,
    near_send, near_recv, alarm_send, alarm_recv,
):
    band, tile = lax.axis_index("band"), lax.axis_index("tile")
    edge = (band == 0) | (band == BANDS - 1)
    chunks = in_sem.shape[0] - 3
    rows = PAIRS // chunks

    def tile_at(k):
        return lax.rem(tile + k, TILES)

    def band_at(k):
        return lax.rem(band + k, BANDS)

    def each_size(body):
        @pl.when(edge)
        def _():
            body(NC, DC)

        @pl.when(jnp.logical_not(edge))
        def _():
            body(NC_MID, DC_MID)

    atm_copy = pltpu.make_async_copy(atm_hbm, atm_ref, in_sem.at[chunks + 1])
    atm_copy.start()
    patch_copy = pltpu.make_async_copy(patch_hbm, patch_ref, in_sem.at[chunks + 2])
    patch_copy.start()
    pat_copy = pltpu.make_async_copy(patches_hbm, pat_v, in_sem.at[chunks])
    pat_copy.start()
    num_copies = [
        pltpu.make_async_copy(
            num_hbm.at[pl.ds(i * rows, rows)], num_v.at[pl.ds(i * rows, rows)], in_sem.at[i]
        )
        for i in range(chunks)
    ]
    for copy in num_copies:
        copy.start()

    barrier = pltpu.get_barrier_semaphore()

    @pl.loop(1, TILES)
    def _(k):
        pl.semaphore_signal(barrier, inc=1, device_id={"tile": tile_at(k)}, device_id_type=MESH)

    @pl.loop(1, BANDS)
    def _(k):
        pl.semaphore_signal(barrier, inc=1, device_id={"band": band_at(k)}, device_id_type=MESH)

    lane, sub = iota((PAIRS, LANES), 1), iota((PAIRS, LANES), 0)
    lane1 = iota((1, LANES), 1)

    def column(row):
        return jnp.sum(jnp.where(lane == sub, row, 0.0), axis=1, keepdims=True)

    atm_copy.wait()
    atm = atm_ref[...]
    live = lane1 < counts_ref[0]
    owner = atm >> 7
    me = band * TILES + tile
    base = jnp.where(
        owner == me,
        0,
        jnp.where(owner == me + TILES, NEAR, jnp.where(owner == me - TILES, 2 * NEAR, FAR0)),
    ).astype(F32)
    key = jnp.where(live, atm, -1).astype(F32)
    key_c, base_c = column(key), column(base)
    same = (key_c == key) & (key >= 0.0)
    earlier = jnp.sum(jnp.where(same & (sub < lane), 1.0, 0.0), axis=0, keepdims=True)
    first = jnp.where(live & (earlier == 0.0), 1.0, 0.0)
    first_c = column(first)
    ahead = (first_c > 0.0) & (base_c == base) & (key_c < key)
    rank = jnp.sum(jnp.where(ahead, 1.0, 0.0), axis=0, keepdims=True)
    slot = jnp.where(live, base + rank, -1.0)
    slot_c = column(slot).astype(I32)
    leads = first_c > 0.0
    later = jnp.sum(jnp.where(same & (sub > lane), 1.0, 0.0), axis=0, keepdims=True)
    last_c = column(jnp.where(live & (later == 0.0), 1.0, 0.0))
    turn = jnp.where(live, slot, 2.0 * PAIRS)
    turn_c = column(turn)
    before = (turn_c < turn) | ((turn_c == turn) & (sub < lane))
    place_c = column(jnp.sum(jnp.where(before, 1.0, 0.0), axis=0, keepdims=True)).astype(I32)
    at = place_c == lane
    table[0:1, :] = jnp.sum(jnp.where(at, sub, 0), axis=0, keepdims=True)
    joins_c = column(earlier).astype(I32)
    table[1:2, :] = jnp.sum(jnp.where(at & (joins_c > 0), 1, 0), axis=0, keepdims=True)
    ends = (last_c > 0.0) & (slot_c == lane)
    table[2:3, :] = PAIRS + jnp.sum(jnp.where(ends, place_c - PAIRS, 0), axis=0, keepdims=True)
    table_copy = pltpu.make_async_copy(table, table_s, table_sem)
    table_copy.start()
    key_i = key_c.astype(I32)
    far_lane = slot_c - FAR0 + NC * lax.rem(tile, 4)
    in_far = leads & (slot_c >= FAR0) & (slot_c < FAR0 + NC)
    far_label = (key_i - band * (TILES * BLOCKS) + 1).astype(F32)
    far_row = jnp.sum(jnp.where(in_far & (far_lane == lane), far_label, 0.0), axis=0, keepdims=True)
    in_near = leads & (slot_c < FAR0) & (slot_c == lane)
    near_label = ((key_i & (BLOCKS - 1)) + 1).astype(F32)
    near_row = jnp.sum(jnp.where(in_near, near_label, 0.0), axis=0, keepdims=True)
    n_far = jnp.sum(jnp.where(base == FAR0, first, 0.0), axis=1, keepdims=True)
    note[0:1, :] = far_row
    note[1:2, :] = jnp.where(lane1 == LANES - 1, n_far, near_row)

    @pl.when(band == 0)
    def _():
        notes[TILES] = jnp.zeros((2, LANES), F32)
        near_ref[1] = jnp.zeros((CELLS * NEAR_STEP, LANES), F32)

    @pl.when(band == BANDS - 1)
    def _():
        notes[TILES + 1] = jnp.zeros((2, LANES), F32)
        near_ref[2] = jnp.zeros((CELLS * NEAR_STEP, LANES), F32)

    @pl.when(jnp.logical_not(edge))
    def _():
        relay[:, :, NC_MID:] = jnp.zeros((TILES, PIECE, NC - NC_MID, LANES), F32)

    @pl.loop(0, CELLS, unroll=4)
    def _(cell):
        far_ref[pl.ds(cell * DC_STEP + DC, 4), :] = jnp.zeros((4, LANES), F32)
        near_ref[0, pl.ds(cell * NEAR_STEP + NEAR, 4), :] = jnp.zeros((4, LANES), F32)
        send_up[pl.ds(cell * NEAR_STEP + NEAR, 4), :] = jnp.zeros((4, LANES), F32)
        send_down[pl.ds(cell * NEAR_STEP + NEAR, 4), :] = jnp.zeros((4, LANES), F32)

    part[PAIRS] = jnp.zeros((CELLS, LANES), F32)

    patch_copy.wait()
    table_copy.wait()
    pat_copy.wait()
    for copy in num_copies:
        copy.wait()

    def add_pair(i, total):
        g = table_s[0, i]
        weight = (num_v[g].astype(F32) * SCALE).astype(BF16)
        product = jnp.dot(weight, pat_v[patch_ref[g]], preferred_element_type=F32)
        total = jnp.where(table_s[1, i] > 0, total, 0.0) + product
        part[i] = total
        return total

    lax.fori_loop(0, PAIRS, add_pair, jnp.zeros((CELLS, LANES), F32), unroll=8)

    @pl.loop(0, NC, unroll=4)
    def _(j):
        send_far[pl.ds(j, CELLS, stride=NC_STEP), :] = part[table_s[2, FAR0 + j]]

    pl.semaphore_wait(barrier, TILES + BANDS - 2)

    def note_to(k):
        return pltpu.make_async_remote_copy(
            src_ref=note, dst_ref=notes.at[tile], send_sem=note_send.at[tile_at(k)],
            recv_sem=note_recv.at[tile], device_id={"tile": tile_at(k)}, device_id_type=MESH,
        )

    def note_from(k):
        source = tile_at(TILES - k)
        return pltpu.make_async_remote_copy(
            src_ref=note, dst_ref=notes.at[source], send_sem=note_send.at[source],
            recv_sem=note_recv.at[source], device_id={"tile": source}, device_id_type=MESH,
        )

    def note_up():
        return pltpu.make_async_remote_copy(
            src_ref=note, dst_ref=notes.at[TILES], send_sem=note_send.at[TILES],
            recv_sem=note_recv.at[TILES], device_id={"band": band_at(1)}, device_id_type=MESH,
        )

    def note_down():
        return pltpu.make_async_remote_copy(
            src_ref=note, dst_ref=notes.at[TILES + 1], send_sem=note_send.at[TILES + 1],
            recv_sem=note_recv.at[TILES + 1], device_id={"band": band_at(BANDS - 1)},
            device_id_type=MESH,
        )

    @pl.loop(1, TILES)
    def _(k):
        note_to(k).start()

    @pl.when(band < BANDS - 1)
    def _():
        note_up().start()

    @pl.when(band > 0)
    def _():
        note_down().start()

    notes[tile] = note[...]

    def far_to(k, c, n):
        return pltpu.make_async_remote_copy(
            src_ref=send_far.at[pl.ds((tile_at(k) * PIECE + c) * NC_STEP, n)], dst_ref=relay.at[tile, c, pl.ds(0, n)],
            send_sem=r_send.at[c, tile_at(k)], recv_sem=r_recv.at[c, tile],
            device_id={"tile": tile_at(k)}, device_id_type=MESH,
        )

    def far_from(k, c, n):
        source = tile_at(TILES - k)
        return pltpu.make_async_remote_copy(
            src_ref=send_far.at[pl.ds((source * PIECE + c) * NC_STEP, n)], dst_ref=relay.at[source, c, pl.ds(0, n)],
            send_sem=r_send.at[c, source], recv_sem=r_recv.at[c, source],
            device_id={"tile": source}, device_id_type=MESH,
        )

    for c in range(PIECE):

        @pl.loop(1, TILES)
        def _(k):
            each_size(lambda n, d: far_to(k, c, n).start())

    for c in range(PIECE):
        relay[tile, c] = send_far[pl.ds((tile * PIECE + c) * NC_STEP, NC), :]

    @pl.loop(0, NEAR, unroll=4)
    def _(j):
        send_up[pl.ds(j, CELLS, stride=NEAR_STEP), :] = part[table_s[2, NEAR + j]]
        send_down[pl.ds(j, CELLS, stride=NEAR_STEP), :] = part[table_s[2, 2 * NEAR + j]]

    def near_up():
        return pltpu.make_async_remote_copy(
            src_ref=send_up, dst_ref=near_ref.at[1], send_sem=near_send.at[0],
            recv_sem=near_recv.at[0], device_id={"band": band_at(1)}, device_id_type=MESH,
        )

    def near_down():
        return pltpu.make_async_remote_copy(
            src_ref=send_down, dst_ref=near_ref.at[2], send_sem=near_send.at[1],
            recv_sem=near_recv.at[1], device_id={"band": band_at(BANDS - 1)}, device_id_type=MESH,
        )

    @pl.when(band < BANDS - 1)
    def _():
        near_up().start()

    @pl.when(band > 0)
    def _():
        near_down().start()

    @pl.loop(0, NEAR, unroll=4)
    def _(j):
        near_ref[0, pl.ds(j, CELLS, stride=NEAR_STEP), :] = part[table_s[2, j]]

    @pl.loop(1, TILES)
    def _(k):
        note_from(k).wait_recv()

    quarters = []
    for q in range(4):
        quarters.append(
            notes[4 * q, 0:1, :] + notes[4 * q + 1, 0:1, :]
            + notes[4 * q + 2, 0:1, :] + notes[4 * q + 3, 0:1, :]
        )
    label = jnp.concatenate(quarters, axis=1).astype(I32)
    entries = TILES * NC
    filled = label > 0
    label = label - 1
    goes_to, block = label >> 7, label & (BLOCKS - 1)
    is_block = filled & (iota((BLOCKS, entries), 0) == block)
    block_hot = jnp.where(is_block, 1.0, 0.0).astype(BF16)
    owner_hot = jnp.where(
        filled & (iota((TILES, entries), 0) == goes_to), 1.0, 0.0
    ).astype(BF16)
    hits = lax.dot_general(
        block_hot, owner_hot, (((1,), (1,)), ((), ())), preferred_element_type=F32
    )
    taken = jnp.where(hits > 0.0, 1.0, 0.0)
    below = jnp.where(lane < sub, 1.0, 0.0).astype(BF16)
    order = jnp.dot(below, taken.astype(BF16), preferred_element_type=F32)
    spread = jnp.dot(order.astype(BF16), owner_hot, preferred_element_type=F32)
    depth = jnp.sum(jnp.where(is_block, spread, 0.0), axis=0, keepdims=True).astype(I32)
    goal = jnp.where(filled & (depth < DC), goes_to * DC + depth, -1)

    most_far = notes[0, 1:2, :]
    for s in range(1, TILES):
        most_far = jnp.maximum(most_far, notes[s, 1:2, :])
    over_far = jnp.max(
        jnp.where(lane1 == LANES - 1, most_far - jnp.where(edge, NC, NC_MID).astype(F32), 0.0), axis=1, keepdims=True
    )
    load = jnp.sum(taken, axis=0, keepdims=True)
    over_load = jnp.max(load - jnp.where(edge, DC, DC_MID).astype(F32), axis=1, keepdims=True)
    alarm[...] = jnp.broadcast_to(
        jnp.where((over_far > 0.0) | (over_load > 0.0), 1.0, 0.0), (1, LANES)
    )

    def alarm_to(k):
        return pltpu.make_async_remote_copy(
            src_ref=alarm, dst_ref=alarms.at[band], send_sem=alarm_send.at[band_at(k)],
            recv_sem=alarm_recv.at[band], device_id={"band": band_at(k)}, device_id_type=MESH,
        )

    def alarm_from(k):
        source = band_at(BANDS - k)
        return pltpu.make_async_remote_copy(
            src_ref=alarm, dst_ref=alarms.at[source], send_sem=alarm_send.at[source],
            recv_sem=alarm_recv.at[source], device_id={"band": source}, device_id_type=MESH,
        )

    @pl.loop(1, BANDS)
    def _(k):
        alarm_to(k).start()

    alarms[band] = alarm[...]

    @pl.when(band > 0)
    def _():
        note_up().wait_recv()

    @pl.when(band < BANDS - 1)
    def _():
        note_down().wait_recv()

    near_labels = jnp.where(
        lane1 < NEAR,
        note[1:2, :],
        jnp.where(lane1 < 2 * NEAR, notes[TILES, 1:2, :], notes[TILES + 1, 1:2, :]),
    )
    here = column(near_labels).astype(I32) == lane + 1
    for i in range(3):
        found = here & (sub >= i * NEAR) & (sub < (i + 1) * NEAR)
        index_ref[i : i + 1, :] = NEAR + jnp.sum(
            jnp.where(found, sub - (i + 1) * NEAR, 0), axis=0, keepdims=True
        )
    mine = iota((BLOCKS, TILES), 1) == tile
    my_row = jnp.sum(
        jnp.where(mine & (taken > 0.0), order - DC, 0.0), axis=1, keepdims=True
    )
    index_ref[3:4, :] = DC + jnp.sum(
        jnp.where(lane == sub, my_row, 0.0), axis=0, keepdims=True
    ).astype(I32)

    index_copy = pltpu.make_async_copy(index_ref, index_s, table_sem)
    index_copy.start()

    depth_sub = iota((GROUP * DC, entries), 0)

    def blocks_of(group, c):
        hot = jnp.where(depth_sub + group * (GROUP * DC) == goal, 1.0, 0.0).astype(BF16)
        return jnp.dot(
            jnp.concatenate([hot, hot], axis=1), stacked[c], preferred_element_type=F32
        ).reshape(GROUP, DC, LANES)

    def parcel_to(target, c, d):
        return pltpu.make_async_remote_copy(
            src_ref=parcel.at[target, c, pl.ds(0, d)],
            dst_ref=far_ref.at[pl.ds((tile * PIECE + c) * DC_STEP, d)],
            send_sem=q_send.at[c, target], recv_sem=q_recv.at[c, tile],
            device_id={"tile": target}, device_id_type=MESH,
        )

    def parcel_from(source, c, d):
        return pltpu.make_async_remote_copy(
            src_ref=parcel.at[source, c, pl.ds(0, d)],
            dst_ref=far_ref.at[pl.ds((source * PIECE + c) * DC_STEP, d)],
            send_sem=q_send.at[c, source], recv_sem=q_recv.at[c, source],
            device_id={"tile": source}, device_id_type=MESH,
        )

    for c in range(PIECE):

        @pl.loop(1, TILES)
        def _(k):
            each_size(lambda n, d: far_from(k, c, n).wait_recv())

        high, low = split(relay[:, c].reshape(entries, LANES))
        stacked[c, :entries] = high
        stacked[c, entries:] = low

        @pl.loop(1, GROUP + 1)
        def _(q):
            group = lax.rem(tile // GROUP + q, GROUP)
            parcel[pl.ds(group * GROUP, GROUP), c] = blocks_of(group, c)

            @pl.loop(0, GROUP)
            def _(k):
                target = group * GROUP + lax.rem(tile + k, GROUP)

                @pl.when(target != tile)
                def _():
                    each_size(lambda n, d: parcel_to(target, c, d).start())

    for c in range(PIECE):
        far_ref[pl.ds((tile * PIECE + c) * DC_STEP, DC), :] = parcel[tile, c]

    @pl.loop(1, BANDS)
    def _(k):
        alarm_from(k).wait_recv()

    index_copy.wait()
    flag_ref[0] = jnp.max(alarms[...]).astype(I32)

    @pl.when(band > 0)
    def _():
        near_up().wait_recv()
        note_down().wait_send()
        near_down().wait_send()

    @pl.when(band < BANDS - 1)
    def _():
        near_down().wait_recv()
        note_up().wait_send()
        near_up().wait_send()

    @pl.loop(1, BANDS)
    def _(k):
        alarm_to(k).wait_send()

    @pl.loop(1, TILES)
    def _(k):
        note_to(k).wait_send()
        for c in range(PIECE):
            each_size(lambda n, d: far_to(k, c, n).wait_send())
            each_size(lambda n, d: parcel_to(tile_at(k), c, d).wait_send())
            each_size(lambda n, d: parcel_from(tile_at(k), c, d).wait_recv())


def exchange(patches, pair_patch, pair_atm, numerators, counts):
    vmem = pl.BlockSpec(memory_space=pltpu.VMEM)
    smem = pl.BlockSpec(memory_space=pltpu.SMEM)
    anywhere = pl.BlockSpec(memory_space=pl.ANY)
    dma = pltpu.SemaphoreType.DMA
    return pl.pallas_call(
        exchange_kernel,
        out_shape=(
            pltpu.VMEM((CELLS * DC_STEP, LANES), F32),
            pltpu.VMEM((3, CELLS * NEAR_STEP, LANES), F32),
            pltpu.SMEM((4, BLOCKS), I32),
            pltpu.SMEM((1,), I32),
        ),
        in_specs=[smem, anywhere, anywhere, anywhere, anywhere],
        out_specs=(vmem, vmem, smem, smem),
        scratch_shapes=[
            pltpu.VMEM((4, BLOCKS), I32),
            pltpu.SMEM((PAIRS,), I32),
            pltpu.VMEM((1, PAIRS), I32),
            pltpu.VMEM((PAIRS, CELLS, LANES), I32),
            pltpu.VMEM((PAIRS // 2, LANES, LANES), BF16),
            pltpu.VMEM((8, PAIRS), I32),
            pltpu.SMEM((8, PAIRS), I32),
            pltpu.VMEM((PAIRS + 1, CELLS, LANES), F32),
            pltpu.VMEM((CELLS * NC_STEP, LANES), F32),
            pltpu.VMEM((CELLS * NEAR_STEP, LANES), F32),
            pltpu.VMEM((CELLS * NEAR_STEP, LANES), F32),
            pltpu.VMEM((TILES, PIECE, NC, LANES), F32),
            pltpu.VMEM((PIECE, 2 * TILES * NC, LANES), BF16),
            pltpu.VMEM((TILES, PIECE, DC, LANES), F32),
            pltpu.VMEM((2, LANES), F32),
            pltpu.VMEM((TILES + 2, 2, LANES), F32),
            pltpu.VMEM((1, LANES), F32),
            pltpu.VMEM((BANDS, 1, LANES), F32),
            dma((7,)), dma,
            dma((TILES + 2,)), dma((TILES + 2,)),
            dma((PIECE, TILES)), dma((PIECE, TILES)),
            dma((PIECE, TILES)), dma((PIECE, TILES)),
            dma((2,)), dma((2,)),
            dma((BANDS,)), dma((BANDS,)),
        ],
        compiler_params=pltpu.CompilerParams(
            collective_id=0, has_side_effects=True, vmem_limit_bytes=24 * 2**20
        ),
        name="exchange",
    )(
        counts,
        pair_patch,
        pair_atm.reshape(1, PAIRS),
        numerators.transpose(0, 2, 1),
        patches.reshape(-1, LANES, LANES),
    )


def place_kernel(index_ref, far_ref, near_ref, out_ref, total, sem):
    parts = sem.shape[0]
    blocks = BLOCKS // parts
    copies = []
    for i in range(parts):

        @pl.loop(i * blocks, (i + 1) * blocks, unroll=4)
        def _(a):
            near = [
                near_ref[r, pl.ds(index_ref[r, a], CELLS, stride=NEAR_STEP), :]
                for r in range(3)
            ]
            far = far_ref[pl.ds(index_ref[3, a], CELLS, stride=DC_STEP), :]
            total[pl.ds(a * CELLS, CELLS), :] = (near[0] + near[1]) + (near[2] + far)

        here = pl.ds(i * blocks * CELLS, blocks * CELLS)
        copies.append(pltpu.make_async_copy(total.at[here], out_ref.at[here], sem.at[i]))
        copies[-1].start()
    for copy in copies:
        copy.wait()


def place(far, near, index):
    vmem = pl.BlockSpec(memory_space=pltpu.VMEM)
    return pl.pallas_call(
        place_kernel,
        out_shape=jax.ShapeDtypeStruct((BLOCKS * CELLS, LANES), F32),
        in_specs=[pl.BlockSpec(memory_space=pltpu.SMEM), vmem, vmem],
        out_specs=pl.BlockSpec(memory_space=pl.ANY),
        scratch_shapes=[
            pltpu.VMEM((BLOCKS * CELLS, LANES), F32),
            pltpu.SemaphoreType.DMA((8,)),
        ],
        compiler_params=pltpu.CompilerParams(vmem_limit_bytes=16 * 2**20),
        name="place",
    )(index, far, near)


def shifted(value, axis, steps):
    count = lax.axis_size(axis)
    first, last = (max(0, -steps), min(count, count - steps))
    return lax.ppermute(value, axis, [(source, source + steps) for source in range(first, last)])


def slot_ranks(owners, blocks_local, live_pairs):
    position = jnp.arange(owners.shape[0])
    earlier = position[None, :] < position[:, None]
    both_live = live_pairs[None, :] & live_pairs[:, None]
    same_owner = (owners[:, None] == owners[None, :]) & both_live
    same_block = same_owner & (blocks_local[:, None] == blocks_local[None, :])
    leading = jnp.logical_not(jnp.any(same_block & earlier, axis=1))
    leader_rank = jnp.sum((same_owner & earlier & leading[None, :]).astype(jnp.int32), axis=1)
    first_match = same_block & leading[None, :]
    return jnp.sum(jnp.where(first_match, leader_rank[None, :], 0), axis=1)


def pack(flattened, rows_index, selected, blocks_local, rows_total):
    onehot = (rows_index[None, :] == jnp.arange(rows_total)[:, None]) & selected[None, :]
    payload = jnp.dot(onehot.astype(jnp.float32), flattened, precision=lax.Precision.HIGHEST)
    labels = jnp.max(jnp.where(onehot, blocks_local[None, :], -1), axis=1)
    return (payload, labels)


def unpack(payload, labels, blocks_owned):
    onehot = (labels[None, :] == jnp.arange(blocks_owned)[:, None]).astype(jnp.float32)
    return jnp.dot(onehot, payload, precision=lax.Precision.HIGHEST)


def along_band(parcel, offset_by):
    return shifted((parcel[0], parcel[1]), "band", offset_by)


def long_route(patches, pair_patch, pair_atm, numerators, counts):
    pairs_here, patch_rows, cell_rows = numerators.shape
    flux_width = patches.shape[1]
    blocks_owned = CELLS_DEV // cell_rows
    capacity = pairs_here // 4
    grouped = patches.reshape(-1, patch_rows, flux_width)
    live_pairs = jnp.arange(pairs_here) < counts[0]
    weight = (numerators.astype(jnp.float32) * SCALE).astype(jnp.bfloat16)
    chosen = grouped[pair_patch]
    partial_value = jnp.einsum("jpa,jpf->jaf", weight, chosen, preferred_element_type=jnp.float32)
    flattened = partial_value.reshape(pairs_here, cell_rows * flux_width)
    owners = pair_atm // blocks_owned
    blocks_local = pair_atm % blocks_owned
    slot_rank = slot_ranks(owners, blocks_local, live_pairs)
    bucket_size = capacity // 2
    tile_count = lax.axis_size("tile")
    band_now = lax.axis_index("band")
    tile_now = lax.axis_index("tile")
    owner_band = owners // tile_count
    owner_tile = owners % tile_count
    in_band = live_pairs & (owner_band == band_now)
    rows_index = jnp.where(in_band, owner_tile * bucket_size + slot_rank, -1)
    payload, labels = pack(flattened, rows_index, in_band, blocks_local, tile_count * bucket_size)

    def bucket(target):
        addressed = live_pairs & (owners == target)
        target_rows = jnp.where(addressed, slot_rank, -1)
        return pack(flattened, target_rows, addressed, blocks_local, bucket_size)

    upper_index = (band_now + 1) * tile_count + tile_now
    lower_index = (band_now - 1) * tile_count + tile_now
    from_below = along_band(bucket(upper_index), 1)
    from_above = along_band(bucket(lower_index), -1)
    band_payload = jnp.concatenate([from_below[0], from_above[0]], axis=0)
    band_labels = jnp.concatenate([from_below[1], from_above[1]], axis=0)
    payload, labels = (
        lax.all_to_all(
            payload.reshape(tile_count, bucket_size, -1),
            "tile",
            split_axis=0,
            concat_axis=0,
            tiled=True,
        ),
        lax.all_to_all(
            labels.reshape(tile_count, bucket_size), "tile", split_axis=0, concat_axis=0, tiled=True
        ),
    )
    payload = jnp.concatenate([payload.reshape(tile_count * bucket_size, -1), band_payload], axis=0)
    labels = jnp.concatenate([labels.reshape(-1), band_labels], axis=0)
    summed = unpack(payload, labels, blocks_owned)
    return summed.reshape(blocks_owned * cell_rows, flux_width)


def per_device(patches, pair_patch, pair_atm, numerators, counts):
    far, near, index, flag = exchange(patches, pair_patch, pair_atm, numerators, counts)
    return lax.cond(
        flag[0] == 0,
        lambda: place(far, near, index),
        lambda: long_route(patches, pair_patch, pair_atm, numerators, counts),
    )


def solution(mesh):
    placed = (
        P(("band", "tile"), None),
        P(("band", "tile")),
        P(("band", "tile")),
        P(("band", "tile"), None, None),
        P(("band", "tile")),
    )
    return jax.shard_map(
        per_device, mesh=mesh, in_specs=placed, out_specs=P(("band", "tile"), None), check_vma=False
    )
```
